32 devices in a mesh: cell: 16 (over z, y, x), gene: 2 (over core).
Axes of the slice: x: 2, y: 2, z: 4, core: 2. Of those that a mesh axis runs over, the one named last changes fastest.
Arguments:
- tiles: bfloat16 [2, 1024, 128, 128], P('gene', 'cell'), may hold values from -8 to 8
- tile_row: int32 [2, 1024], P('gene', 'cell'), may hold values from 0 to 7, as said below
- tile_col: int32 [2, 1024], P('gene', 'cell'), may hold values from 0 to 15
- tile_count: int32 [2, 16], P('gene', 'cell'), may hold values from 1 to 64, as said below
- start_basis: bfloat16 [64, 4096], P(None, 'gene'), may hold values from -0.09375 to 0.09375
Outputs:
- basis: bfloat16 [64, 16384], P(None, 'cell')
- loadings: float32 [64, 4096], P(None, ('gene', 'cell'))
The draws below stay inside these ranges and needn't reach their ends.
Inputs may be any that keep to these rules, and one draw needn't show every extreme that they name: `tile_row`: tile row of each slot, within 0 to 7; the slots of one device name distinct (row, column) pairs. `tile_count`: slots in use; for each index of gene some device uses all 64.
All inputs are finite; a program needn't handle non-finite values.
Results may differ from the reference program's by a relative error of at most 0.018.
Values may be sent and summed in bfloat16 or wider, within the bound.
A program may use at most 64 MiB of HBM per device.

```python
import jax
import jax.numpy as jnp
from jax import lax

K = 64
G = 4096
TILE = 128
ROW_BLOCKS = 8
N_CELL = 16
N_GENE = 2


strongest = 32.0


tile_scale = 0.125


def slot_places(key):
    base = jax.random.fold_in(key, 7)
    gene_blocks = G // (N_GENE * TILE)
    slot_count = ROW_BLOCKS * gene_blocks // 2
    keys = jax.random.split(base, N_GENE * N_CELL)

    def one_device(device_key):
        return jax.random.permutation(device_key, ROW_BLOCKS * gene_blocks)[:slot_count].astype(jnp.int32)
    places = jax.vmap(one_device)(keys)
    return (places.reshape(N_GENE, N_CELL * slot_count), gene_blocks)


def draw_tiles(key, part):
    places, gene_blocks = slot_places(key)
    slot_count = ROW_BLOCKS * gene_blocks // 2
    columns_all = G // TILE
    per_column = (K + columns_all - 1) // columns_all
    row_local = places // gene_blocks
    col_local = places % gene_blocks
    gene_of = jnp.arange(N_GENE, dtype=jnp.int32)[:, None]
    cell_of = (jnp.arange(N_CELL * slot_count, dtype=jnp.int32) // slot_count)[None, :]
    global_col = (gene_of * gene_blocks + col_local).reshape(N_GENE * N_CELL, slot_count).astype(jnp.int32)
    global_row = (cell_of * ROW_BLOCKS + row_local).reshape(N_GENE * N_CELL, slot_count).astype(jnp.int32)
    ladder = strongest ** (jnp.arange(K, dtype=jnp.float32) / jnp.float32(K - 1))
    order = jax.random.permutation(jax.random.fold_in(key, 21), K)
    strength = ladder[order]
    component = jnp.arange(columns_all, dtype=jnp.int32)[:, None] + columns_all * jnp.arange(per_column, dtype=jnp.int32)[None, :]
    column_strength = jnp.where(component < K, strength[jnp.minimum(component, K - 1)], 0.0)
    gene_factor = jax.random.truncated_normal(jax.random.fold_in(key, 23), -3.0, 3.0, (columns_all, per_column, TILE), jnp.float32)
    gene_factor = gene_factor / jnp.sqrt(jnp.float32(TILE))
    cell_key = jax.random.fold_in(key, 27)
    noise_key = jax.random.fold_in(key, 25)
    rise_ratio = 3.0

    def one_device(index):
        columns = global_col[index]
        rows = global_row[index]
        cell_index = (index % N_CELL).astype(jnp.float32)
        rise = jnp.float32(rise_ratio) ** (cell_index / jnp.float32(max(N_CELL - 1, 1)))
        slot_keys = jax.vmap(lambda row, col: jax.random.fold_in(cell_key, row * columns_all + col))(rows, columns)
        device_key = jax.random.fold_in(noise_key, index)
        cell_factor = jax.vmap(lambda one_key: jax.random.truncated_normal(one_key, -3.0, 3.0, (per_column, TILE), jnp.float32))(slot_keys)
        noise = jax.random.truncated_normal(device_key, -4.0, 4.0, (slot_count, TILE, TILE), jnp.float32)
        weighted = cell_factor * column_strength[columns][:, :, None]
        planted = jnp.einsum('spr,spg->srg', weighted, gene_factor[columns])
        return jnp.clip(tile_scale * rise * (noise + planted), -8.0, 8.0).astype(jnp.bfloat16)
    stacked = lax.map(one_device, jnp.arange(N_GENE * N_CELL, dtype=jnp.int32))
    return stacked.reshape(N_GENE, N_CELL * slot_count, TILE, TILE)


def draw_tile_row(key, part):
    places, gene_blocks = slot_places(key)
    return (places // gene_blocks).astype(jnp.int32)


def draw_tile_col(key, part):
    places, gene_blocks = slot_places(key)
    return (places % gene_blocks).astype(jnp.int32)


def draw_tile_count(key, part):
    slot_count = ROW_BLOCKS * (G // (N_GENE * TILE)) // 2
    first_key, second_key = jax.random.split(jax.random.fold_in(key, 11))
    lowest = max(1, slot_count // 8)
    highest = max(lowest + 1, slot_count * 7 // 8 + 1)
    counts = jax.random.randint(first_key, (N_GENE, N_CELL), lowest, highest, dtype=jnp.int32)
    fullest = jax.random.randint(second_key, (N_GENE, 1), 0, N_CELL, dtype=jnp.int32)
    return jnp.where(jnp.arange(N_CELL, dtype=jnp.int32)[None, :] == fullest, slot_count, counts).astype(jnp.int32)


def block_scale(key, shape, pieces, least, high):
    gain = 1.0
    for dim, blocks in pieces:
        steps = jax.random.uniform(jax.random.fold_in(jax.random.fold_in(key, 6), dim), (blocks,), jnp.float32, least / len(pieces), high / len(pieces))
        gain = gain * jnp.repeat(jnp.exp(steps), shape[dim] // blocks).reshape((-1,) + (1,) * (len(shape) - 1 - dim))
    return gain


def scatter_about(key, extent, width, bound, cuts=(), kind=jnp.bfloat16):
    values = jax.random.normal(key, extent, jnp.float32) * width
    if len(cuts) > 0:
        values = block_scale(key, extent, cuts, -0.22, 0.18) * values
    return jnp.clip(values, min=-bound, max=bound).astype(kind)


def setup_inputs(seed: int = 0) -> dict:
    key_list = jax.random.split(jax.random.key(seed), 6)
    tiles = draw_tiles(jax.random.fold_in(key_list[5], 71), 0)
    tile_row = draw_tile_row(jax.random.fold_in(key_list[5], 71), 0)
    tile_col = draw_tile_col(jax.random.fold_in(key_list[5], 71), 0)
    tile_count = draw_tile_count(jax.random.fold_in(key_list[5], 71), 0)
    start_basis = scatter_about(key_list[4], (K, G), G ** -0.5, 0.09375, ((1, 2),))
    return {"tiles": tiles, "tile_row": tile_row, "tile_col": tile_col, "tile_count": tile_count, "start_basis": start_basis}


def solve_lower(lower, right):
    return lax.linalg.triangular_solve(lower, right, left_side=True, lower=True)

def gram_of(scores):
    return jnp.dot(scores.astype(jnp.float32), scores.T.astype(jnp.float32), precision=lax.Precision.HIGHEST, preferred_element_type=jnp.float32)

def orthonormal(scores):
    lower_one = jnp.linalg.cholesky(gram_of(scores))
    return solve_lower(lower_one, scores)

def reference(tiles, tile_row, tile_col, tile_count, start_basis):
    slot_count = tiles.shape[1] // N_CELL
    gene_dev = G // N_GENE
    gene_blocks = gene_dev // TILE
    cell_dev = ROW_BLOCKS * TILE
    grouped = tiles.reshape(N_GENE, N_CELL, slot_count, TILE, TILE)
    rows_all = tile_row.reshape(N_GENE, N_CELL, slot_count)
    cols_all = tile_col.reshape(N_GENE, N_CELL, slot_count)

    def onehots(gene, cell):
        live_mask = (jnp.arange(slot_count) < tile_count[gene, cell]).astype(jnp.float32)
        row_hot = (rows_all[gene, cell][:, None] == jnp.arange(ROW_BLOCKS)[None, :]).astype(jnp.float32) * live_mask[:, None]
        col_hot = (cols_all[gene, cell][:, None] == jnp.arange(gene_blocks)[None, :]).astype(jnp.float32) * live_mask[:, None]
        return (row_hot, col_hot)

    def scores_of(basis):

        def one_cell(cell):
            total = jnp.zeros((K, cell_dev), jnp.float32)
            for gene in range(N_GENE):
                row_hot, col_hot = onehots(gene, cell)
                local = basis[:, gene * gene_dev:(gene + 1) * gene_dev].reshape(K, gene_blocks, TILE)
                picked = jnp.take(local, cols_all[gene, cell], axis=1).astype(jnp.float32)
                products = jnp.einsum('ksg,srg->skr', picked, grouped[gene, cell].astype(jnp.float32), precision=lax.Precision.HIGHEST)
                summed = jnp.einsum('sb,skr->kbr', row_hot, products, precision=lax.Precision.HIGHEST)
                total = total + summed.reshape(K, cell_dev)
            return total
        stacked = lax.map(one_cell, jnp.arange(N_CELL))
        return jnp.transpose(stacked, (1, 0, 2)).reshape(K, N_CELL * cell_dev)

    def loadings_of(ortho_half):
        blocks = ortho_half.reshape(K, N_CELL, cell_dev)

        def step(carry, cell):
            parts = []
            for gene in range(N_GENE):
                row_hot, col_hot = onehots(gene, cell)
                local = blocks[:, cell].reshape(K, ROW_BLOCKS, TILE)
                picked = jnp.take(local, rows_all[gene, cell], axis=1).astype(jnp.float32)
                products = jnp.einsum('ksr,srg->skg', picked, grouped[gene, cell].astype(jnp.float32), precision=lax.Precision.HIGHEST)
                summed = jnp.einsum('sb,skg->kbg', col_hot, products, precision=lax.Precision.HIGHEST)
                parts.append(summed.reshape(K, gene_dev))
            return (carry + jnp.stack(parts), None)
        start = jnp.zeros((N_GENE, K, gene_dev), jnp.float32)
        total, _ = lax.scan(step, start, jnp.arange(N_CELL))
        return jnp.transpose(total, (1, 0, 2)).reshape(K, G)
    ortho = orthonormal(scores_of(start_basis))
    middle = loadings_of(ortho.astype(jnp.bfloat16))
    ortho_two = orthonormal(scores_of(middle.astype(jnp.bfloat16)))
    loadings = loadings_of(ortho_two.astype(jnp.bfloat16))
    basis = (ortho_two * jnp.sqrt(jnp.float32(N_CELL * cell_dev))).astype(jnp.bfloat16)
    return (basis, loadings)
```

```python
import functools

import jax
import jax.numpy as jnp
from jax import lax
from jax.experimental import pallas as pl
from jax.experimental.pallas import tpu as pltpu
from jax.sharding import PartitionSpec as P

ROW_BLOCKS = 8
PANEL = 4
MESH = pl.DeviceIdType.MESH
HIGH = lax.Precision.HIGHEST


def split_three(value):
    high = value.astype(jnp.bfloat16)
    rest = value - high.astype(jnp.float32)
    middle = rest.astype(jnp.bfloat16)
    low = (rest - middle.astype(jnp.float32)).astype(jnp.bfloat16)
    return high, middle, low


def inverse_factor(gram):
    width = gram.shape[0]
    shape = (width, 2 * width)
    row = lax.broadcasted_iota(jnp.int32, shape, 0)
    lane = lax.broadcasted_iota(jnp.int32, shape, 1)
    both = jnp.concatenate([jnp.zeros_like(gram), gram], axis=1)
    both = jnp.where(row == lane, 1.0, both)
    pivots = jnp.ones(shape, jnp.float32)
    done = []
    start = 0

    def spread(first):
        return {
            j: jnp.broadcast_to(both[:, width + j : width + j + 1], both.shape)
            for j in range(first, min(first + PANEL, width))
        }

    ahead = spread(0)
    for first in range(0, width, PANEL):
        base = first // 8 * 8
        if base > start:
            done.append((both[: base - start], pivots[: base - start]))
            both = both[base - start :]
            pivots = pivots[base - start :]
            row = row[base - start :]
            ahead = {j: column[base - start :] for j, column in ahead.items()}
            start = base
        columns = ahead
        ahead = spread(first + PANEL)
        for j in range(first, first + PANEL):
            at = j - start
            column = columns.pop(j)
            pivot = column[at : at + 1]
            factor = jnp.where(row > j, column * (1.0 / pivot), 0.0)
            pivots = jnp.where(row == j, pivot, pivots)
            both = both - factor * both[at : at + 1]
            for later in (columns, ahead):
                for m in later:
                    later[m] = later[m] - factor * later[m][at : at + 1]
    done.append((both, pivots))
    both = jnp.concatenate([piece for piece, _ in done], axis=0)
    pivots = jnp.concatenate([piece for _, piece in done], axis=0)
    return (both * lax.rsqrt(pivots))[:, :width]


def kernel(
    cells, inner, genes, parts,
    slot_count, slot_row, slot_col, tiles, start, basis_out, load_out,
    rows_in, cols_in, places_out, table, held, dense, mine, theirs, stacked, grams, planes, sums_out, sums_mid, sums_own, sums_in, middle, basis,
    tile_sem, slot_sem, table_sem, start_sem, pair_send, pair_recv, gram_send, gram_recv, plane_send, plane_recv,
    near_send, near_recv, far_send, far_recv, mid_send, mid_recv,
):
    cell = lax.axis_index("cell")
    gene = lax.axis_index("gene")
    slots, side, _ = tiles.shape
    width = start.shape[0]
    cell_dev, gene_dev = dense.shape
    gene_blocks = gene_dev // side
    chunk = gene_dev // cells
    piece = cell_dev // parts
    half = width // 2
    outer = cells // inner
    here = cell // inner
    spot = lax.rem(cell, inner)
    other = lax.rem(gene + 1, genes)

    slot_copies = [
        pltpu.make_async_copy(slot_row, rows_in, slot_sem.at[0]),
        pltpu.make_async_copy(slot_col, cols_in, slot_sem.at[1]),
    ]
    for copy in slot_copies:
        copy.start()
    fetch = pltpu.make_async_copy(tiles, held.at[pl.ds(0, slots)], tile_sem)
    fetch.start()
    first_basis = pltpu.make_async_copy(start, basis, start_sem)
    first_basis.start()

    barrier = pltpu.get_barrier_semaphore()

    def greet(k, _):
        pl.semaphore_signal(
            barrier, inc=1, device_id={"cell": lax.rem(cell + k, cells)}, device_id_type=MESH
        )
        return 0

    pl.semaphore_signal(barrier, inc=1, device_id={"gene": other}, device_id_type=MESH)
    lax.fori_loop(1, cells, greet, 0)
    held[slots] = jnp.zeros((side, side), held.dtype)
    for copy in slot_copies:
        copy.wait()
    places = (cell_dev // side) * gene_blocks
    lane = lax.broadcasted_iota(jnp.int32, (1, slots), 1)
    spots = jnp.where(lane < slot_count[0, 0], rows_in[...] * gene_blocks + cols_in[...], places)
    square = (slots, slots)
    turned = jnp.where(
        lax.broadcasted_iota(jnp.int32, square, 0) == lax.broadcasted_iota(jnp.int32, square, 1),
        jnp.broadcast_to(spots, square), 0,
    )
    turned = jnp.sum(turned, axis=1, keepdims=True)
    flat = (slots, places)
    found = jnp.broadcast_to(turned, flat) == lax.broadcasted_iota(jnp.int32, flat, 1)
    found = jnp.where(found, lax.broadcasted_iota(jnp.int32, flat, 0), slots)
    places_out[...] = jnp.min(found, axis=0, keepdims=True)
    listing = pltpu.make_async_copy(places_out, table, table_sem)
    listing.start()
    listing.wait()
    fetch.wait()

    def place(row, _):
        for col in range(gene_blocks):
            dense[
                pl.ds(pl.multiple_of(row * side, side), side), col * side : (col + 1) * side
            ] = held[table[0, row * gene_blocks + col]]
        return 0

    lax.fori_loop(0, cell_dev // side, place, 0)
    first_basis.wait()
    pl.semaphore_wait(barrier, cells)

    def pair_copy(it, r):
        return pltpu.make_async_remote_copy(
            src_ref=mine.at[it, r], dst_ref=theirs.at[it, r],
            send_sem=pair_send.at[it, r], recv_sem=pair_recv.at[it, r],
            device_id={"gene": other}, device_id_type=MESH,
        )

    def near(k):
        return here * inner + lax.rem(spot + k, inner)

    def far(k):
        return lax.rem(here + k, outer) * inner + spot

    def gram_copy(it, source, k):
        return pltpu.make_async_remote_copy(
            src_ref=grams.at[it, source], dst_ref=grams.at[it, source],
            send_sem=gram_send.at[it, k], recv_sem=gram_recv.at[it, source],
            device_id={"cell": near(k)}, device_id_type=MESH,
        )

    def plane_copy(it, source, k):
        return pltpu.make_async_remote_copy(
            src_ref=planes.at[it, source], dst_ref=planes.at[it, source],
            send_sem=plane_send.at[it, k], recv_sem=plane_recv.at[it, source],
            device_id={"cell": far(k)}, device_id_type=MESH,
        )

    def near_copy(it, group, source, k):
        return pltpu.make_async_remote_copy(
            src_ref=sums_out.at[it, group, lax.rem(spot + k, inner)],
            dst_ref=sums_mid.at[it, group, source],
            send_sem=near_send.at[it, group, k], recv_sem=near_recv.at[it, group, source],
            device_id={"cell": near(k)}, device_id_type=MESH,
        )

    def far_copy(it, source, k):
        return pltpu.make_async_remote_copy(
            src_ref=sums_own.at[it, lax.rem(here + k, outer)], dst_ref=sums_in.at[it, source],
            send_sem=far_send.at[it, k], recv_sem=far_recv.at[it, source],
            device_id={"cell": far(k)}, device_id_type=MESH,
        )

    def mid_copy(source, k):
        return pltpu.make_async_remote_copy(
            src_ref=middle.at[source], dst_ref=middle.at[source],
            send_sem=mid_send.at[k], recv_sem=mid_recv.at[source],
            device_id={"cell": lax.rem(cell + k, cells)}, device_id_type=MESH,
        )

    def each(act):
        def body(k, _):
            act(lax.rem(cell + cells - k, cells), k)
            return 0

        lax.fori_loop(1, cells, body, 0)

    def farther(k):
        return lax.rem(k + cells // 2, cells)

    def each_near(act):
        for k in range(1, inner):
            act(lax.rem(spot + inner - k, inner), k)

    def each_far(act):
        for k in range(1, outer):
            act(lax.rem(here + outer - k, outer), k)

    def added(ref, count):
        total = ref[0]
        for c in range(1, count):
            total = total + ref[c]
        return total

    def loop(first, last, act):
        def body(k, _):
            act(k)
            return 0

        lax.fori_loop(first, last, body, 0)

    def part(r):
        return pl.ds(pl.multiple_of(r * piece, piece), piece)

    def iteration(it):
        def score(r):
            mine[it, r] = lax.dot_general(
                basis[...], dense[part(r), :], (((1,), (1,)), ((), ())),
                preferred_element_type=jnp.float32,
            )
            pair_copy(it, r).start()

        def merge(r):
            pair_copy(it, r).wait_recv()
            high, mid, low = split_three(mine[it, r] + theirs[it, r])
            stacked[0:width, part(r)] = high
            stacked[width : 2 * width, part(r)] = mid
            stacked[2 * width : 3 * width, part(r)] = low

        loop(0, parts, score)
        loop(0, parts, merge)

        whole = stacked[...]
        cross = lax.dot_general(
            whole, whole, (((1,), (1,)), ((), ())), preferred_element_type=jnp.float32
        )
        cross = cross[:width] + cross[width : 2 * width] + cross[2 * width :]
        gram = cross[:, :width] + cross[:, width : 2 * width] + cross[:, 2 * width :]
        grams[it, spot] = jnp.concatenate([gram[:half], gram[half:]], axis=1)
        each_near(lambda _, k: gram_copy(it, spot, k).start())

        def product(columns):
            pair = jnp.dot(
                stacked[0 : 2 * width, :], columns, preferred_element_type=jnp.float32
            )
            return pair[:width] + pair[width:]

        span = inner * chunk

        def multiply(k):
            group = lax.rem(here + k, outer)
            if span % 128 == 0:
                wide = product(dense[:, pl.ds(pl.multiple_of(group * span, 128), span)])
                for c in range(inner):
                    sums_out[it, group, c] = wide[:, c * chunk : (c + 1) * chunk]
            each_near(lambda _, k: near_copy(it, group, spot, k).start())

        def forward(k):
            group = lax.rem(here + k, outer)
            each_near(lambda source, k: near_copy(it, group, source, k).wait_recv())
            total = sums_out[it, group, spot]
            for c in range(1, inner):
                total = total + sums_mid[it, group, lax.rem(spot + c, inner)]
            if isinstance(k, int):
                sums_in[it, here] = total
            else:
                sums_own[it, group] = total
                far_copy(it, here, k).start()

        if span % 128 != 0:
            for b in range(gene_blocks):
                wide = product(dense[:, b * side : (b + 1) * side])
                for c in range(side // chunk):
                    at = b * (side // chunk) + c
                    sums_out[it, at // inner, at % inner] = wide[:, c * chunk : (c + 1) * chunk]
        multiply(1)
        each_near(lambda source, k: gram_copy(it, source, k).wait_recv())
        planes[it, here] = added(grams.at[it], inner)
        each_far(lambda _, k: plane_copy(it, here, k).start())
        loop(2, outer + 1, multiply)
        loop(1, outer, forward)
        each_far(lambda source, k: plane_copy(it, source, k).wait_recv())
        total = added(planes.at[it], outer)
        total = jnp.concatenate([total[:, :width], total[:, width:]], axis=0)
        inverse = inverse_factor(total)

        @pl.when(it == 1)
        def _():
            scale = jnp.sqrt(jnp.float32(cells * cell_dev))

            def finish(r):
                basis_out[:, part(r)] = (
                    jnp.dot(
                        inverse, mine[it, r] + theirs[it, r], precision=HIGH,
                        preferred_element_type=jnp.float32,
                    ) * scale
                ).astype(basis_out.dtype)

            loop(0, parts, finish)

        forward(0)
        each_far(lambda source, k: far_copy(it, source, k).wait_recv())
        summed = added(sums_in.at[it], outer)
        result = jnp.dot(inverse, summed, precision=HIGH, preferred_element_type=jnp.float32)

        @pl.when(it == 0)
        def _():
            middle[cell] = result.astype(middle.dtype)
            each(lambda _, k: mid_copy(cell, k).start())
            each(lambda source, k: mid_copy(source, k).wait_recv())
            basis[...] = jnp.concatenate([middle[c] for c in range(cells)], axis=1)

        @pl.when(it == 1)
        def _():
            load_out[...] = result

    loop(0, 2, iteration)

    def drain(it):
        loop(0, parts, lambda r: pair_copy(it, r).wait_send())
        each_near(lambda _, k: gram_copy(it, spot, k).wait_send())
        each_far(lambda _, k: plane_copy(it, here, k).wait_send())
        loop(0, outer, lambda group: each_near(lambda _, k: near_copy(it, group, spot, k).wait_send()))
        each_far(lambda _, k: far_copy(it, here, k).wait_send())

    loop(0, 2, drain)
    each(lambda _, k: mid_copy(cell, k).wait_send())


def local(cells, genes, tiles, tile_row, tile_col, tile_count, start_basis):
    slots, side = tiles.shape[1], tiles.shape[-1]
    width, gene_dev = start_basis.shape
    gene_blocks = gene_dev // side
    cell_dev = ROW_BLOCKS * side
    chunk = gene_dev // cells
    parts = 4
    inner = 1
    while inner * inner * 4 <= cells and cells % (inner * 2) == 0:
        inner = inner * 2
    outer = cells // inner
    places = ROW_BLOCKS * gene_blocks
    dma = pltpu.SemaphoreType.DMA
    return pl.pallas_call(
        functools.partial(kernel, cells, inner, genes, parts),
        out_shape=(
            jax.ShapeDtypeStruct((width, cell_dev), jnp.bfloat16),
            jax.ShapeDtypeStruct((width, chunk), jnp.float32),
        ),
        in_specs=[
            pl.BlockSpec(memory_space=pltpu.SMEM),
            pl.BlockSpec(memory_space=pltpu.HBM),
            pl.BlockSpec(memory_space=pltpu.HBM),
            pl.BlockSpec(memory_space=pltpu.HBM),
            pl.BlockSpec(memory_space=pltpu.HBM),
        ],
        out_specs=(
            pl.BlockSpec(memory_space=pltpu.VMEM),
            pl.BlockSpec(memory_space=pltpu.VMEM),
        ),
        scratch_shapes=[
            pltpu.VMEM((1, slots), jnp.int32),
            pltpu.VMEM((1, slots), jnp.int32),
            pltpu.VMEM((1, places), jnp.int32),
            pltpu.SMEM((1, places), jnp.int32),
            pltpu.VMEM((slots + 1, side, side), jnp.bfloat16),
            pltpu.VMEM((cell_dev, gene_dev), jnp.bfloat16),
            pltpu.VMEM((2, parts, width, cell_dev // parts), jnp.float32),
            pltpu.VMEM((2, parts, width, cell_dev // parts), jnp.float32),
            pltpu.VMEM((3 * width, cell_dev), jnp.bfloat16),
            pltpu.VMEM((2, inner, width // 2, 2 * width), jnp.float32),
            pltpu.VMEM((2, outer, width // 2, 2 * width), jnp.float32),
            pltpu.VMEM((2, outer, inner, width, chunk), jnp.float32),
            pltpu.VMEM((2, outer, inner, width, chunk), jnp.float32),
            pltpu.VMEM((2, outer, width, chunk), jnp.float32),
            pltpu.VMEM((2, outer, width, chunk), jnp.float32),
            pltpu.VMEM((cells, width, chunk), jnp.bfloat16),
            pltpu.VMEM((width, gene_dev), jnp.bfloat16),
            dma, dma((2,)), dma, dma,
            dma((2, parts)), dma((2, parts)),
            dma((2, inner)), dma((2, inner)), dma((2, outer)), dma((2, outer)),
            dma((2, outer, inner)), dma((2, outer, inner)), dma((2, outer)), dma((2, outer)),
            dma((cells,)), dma((cells,)),
        ],
        compiler_params=pltpu.CompilerParams(
            collective_id=0, has_side_effects=True, vmem_limit_bytes=36 * 1024 * 1024
        ),
    )(tile_count, *(
        pltpu.with_memory_space_constraint(array, pltpu.HBM)
        for array in (tile_row, tile_col, tiles[0], start_basis)
    ))


def solution(mesh):
    return jax.shard_map(
        functools.partial(local, mesh.shape["cell"], mesh.shape["gene"]),
        mesh=mesh,
        in_specs=(
            P("gene", "cell", None, None),
            P("gene", "cell"),
            P("gene", "cell"),
            P("gene", "cell"),
            P(None, "gene"),
        ),
        out_specs=(P(None, "cell"), P(None, ("gene", "cell"))),
        check_vma=False,
    )
```

```python
import functools

import jax
import jax.numpy as jnp
from jax import lax
from jax.experimental import pallas as pl
from jax.experimental.pallas import tpu as pltpu
from jax.sharding import PartitionSpec as P

ROW_BLOCKS = 8
PANEL = 4
LEVELS = 32766.0
MESH = pl.DeviceIdType.MESH
HIGH = lax.Precision.HIGHEST
scope = jax.named_scope


def split_three(value):
    high = value.astype(jnp.bfloat16)
    rest = value - high.astype(jnp.float32)
    middle = rest.astype(jnp.bfloat16)
    low = (rest - middle.astype(jnp.float32)).astype(jnp.bfloat16)
    return high, middle, low


def inverse_factor(gram):
    width = gram.shape[0]
    shape = (width, 2 * width)
    row = lax.broadcasted_iota(jnp.int32, shape, 0)
    lane = lax.broadcasted_iota(jnp.int32, shape, 1)
    both = jnp.concatenate([jnp.zeros_like(gram), gram], axis=1)
    both = jnp.where(row == lane, 1.0, both)
    pivots = jnp.ones(shape, jnp.float32)
    done = []
    start = 0

    def spread(first):
        return {
            j: jnp.broadcast_to(both[:, width + j : width + j + 1], both.shape)
            for j in range(first, min(first + PANEL, width))
        }

    ahead = spread(0)
    for first in range(0, width, PANEL):
        base = first // 8 * 8
        if base > start:
            done.append((both[: base - start], pivots[: base - start]))
            both = both[base - start :]
            pivots = pivots[base - start :]
            row = row[base - start :]
            ahead = {j: column[base - start :] for j, column in ahead.items()}
            start = base
        columns = ahead
        ahead = spread(first + PANEL)
        for j in range(first, first + PANEL):
            at = j - start
            column = columns.pop(j)
            pivot = column[at : at + 1]
            factor = jnp.where(row > j, column * (1.0 / pivot), 0.0)
            pivots = jnp.where(row == j, pivot, pivots)
            both = both - factor * both[at : at + 1]
            for later in (columns, ahead):
                for m in later:
                    later[m] = later[m] - factor * later[m][at : at + 1]
    done.append((both, pivots))
    both = jnp.concatenate([piece for piece, _ in done], axis=0)
    pivots = jnp.concatenate([piece for _, piece in done], axis=0)
    return (both * lax.rsqrt(pivots))[:, :width]


def diagonal(width):
    square = (width, width)
    return lax.broadcasted_iota(jnp.int32, square, 0) == lax.broadcasted_iota(jnp.int32, square, 1)


def encode(value):
    peak = jnp.max(jnp.abs(value), axis=1, keepdims=True)
    step = jnp.maximum(peak, 1e-30) * (1.0 / LEVELS)
    coded = jnp.round(value * (1.0 / step)).astype(jnp.int32).astype(jnp.int16)
    square = (value.shape[0], value.shape[0])
    turned = jnp.where(diagonal(square[0]), jnp.broadcast_to(step, square), 0.0)
    return coded, jnp.sum(turned, axis=0, keepdims=True)


def decode(coded, steps):
    square = (coded.shape[0], coded.shape[0])
    turned = jnp.where(diagonal(square[0]), jnp.broadcast_to(steps, square), 0.0)
    step = jnp.sum(turned, axis=1, keepdims=True)
    return coded.astype(jnp.int32).astype(jnp.float32) * step


def kernel(
    cells, inner, genes, parts,
    slot_count, slot_row, slot_col, tiles, start, basis_out, load_out,
    rows_in, cols_in, places_out, table, held, dense, first, mine, theirs, stacked, grams, planes, totals,
    sums_near, codes_out, codes_in, steps_out, steps_in, sums_own, sums_in, middle,
    tile_sem, slot_sem, table_sem, start_sem, pair_send, pair_recv,
    gram_send, gram_recv, plane_send, plane_recv, total_send, total_recv,
    near_send, near_recv, step_send, step_recv, far_send, far_recv, mid_send, mid_recv,
):
    cell = lax.axis_index("cell")
    gene = lax.axis_index("gene")
    slots, side, _ = tiles.shape
    width = start.shape[0]
    cell_dev, gene_dev = dense.shape
    gene_blocks = gene_dev // side
    chunk = gene_dev // cells
    piece = cell_dev // parts
    half = width // 2
    outer = cells // inner
    span = inner * chunk
    here = cell // inner
    spot = lax.rem(cell, inner)
    other = lax.rem(gene + 1, genes)
    lead = gene == genes - 1

    slot_copies = [
        pltpu.make_async_copy(slot_row, rows_in, slot_sem.at[0]),
        pltpu.make_async_copy(slot_col, cols_in, slot_sem.at[1]),
    ]
    for copy in slot_copies:
        copy.start()
    fetch = pltpu.make_async_copy(tiles, held.at[pl.ds(0, slots)], tile_sem)
    fetch.start()
    first_basis = pltpu.make_async_copy(start, first, start_sem)
    first_basis.start()

    barrier = pltpu.get_barrier_semaphore()

    def greet(k, _):
        pl.semaphore_signal(
            barrier, inc=1, device_id={"cell": lax.rem(cell + k, cells)}, device_id_type=MESH
        )
        return 0

    pl.semaphore_signal(barrier, inc=1, device_id={"gene": other}, device_id_type=MESH)
    lax.fori_loop(1, cells, greet, 0)
    held[slots] = jnp.zeros((side, side), held.dtype)
    for copy in slot_copies:
        copy.wait()
    places = (cell_dev // side) * gene_blocks
    lane = lax.broadcasted_iota(jnp.int32, (1, slots), 1)
    spots = jnp.where(
        lane < slot_count[0, 0], rows_in[...] * gene_blocks + cols_in[...], places
    )
    square = (slots, slots)
    turned = jnp.where(diagonal(slots), jnp.broadcast_to(spots, square), 0)
    turned = jnp.sum(turned, axis=1, keepdims=True)
    flat = (slots, places)
    found = jnp.broadcast_to(turned, flat) == lax.broadcasted_iota(jnp.int32, flat, 1)
    found = jnp.where(found, lax.broadcasted_iota(jnp.int32, flat, 0), slots)
    places_out[...] = jnp.min(found, axis=0, keepdims=True)
    listing = pltpu.make_async_copy(places_out, table, table_sem)
    listing.start()
    listing.wait()
    fetch.wait()
    first_basis.wait()

    def pair_copy(it, r):
        return pltpu.make_async_remote_copy(
            src_ref=mine.at[it, r], dst_ref=theirs.at[it, r],
            send_sem=pair_send.at[it, r], recv_sem=pair_recv.at[it, r],
            device_id={"gene": other}, device_id_type=MESH,
        )

    def near(k):
        return here * inner + lax.rem(spot + k, inner)

    def far(k):
        return lax.rem(here + k, outer) * inner + spot

    def gram_copy(it, source, k):
        return pltpu.make_async_remote_copy(
            src_ref=grams.at[it, source], dst_ref=grams.at[it, source],
            send_sem=gram_send.at[it, k], recv_sem=gram_recv.at[it, source],
            device_id={"cell": near(k)}, device_id_type=MESH,
        )

    def plane_copy(it, source, k):
        return pltpu.make_async_remote_copy(
            src_ref=planes.at[it, source], dst_ref=planes.at[it, source],
            send_sem=plane_send.at[it, k], recv_sem=plane_recv.at[it, source],
            device_id={"cell": far(k)}, device_id_type=MESH,
        )

    def total_copy(it):
        return pltpu.make_async_remote_copy(
            src_ref=totals.at[it], dst_ref=totals.at[it],
            send_sem=total_send.at[it], recv_sem=total_recv.at[it],
            device_id={"gene": other}, device_id_type=MESH,
        )

    def near_copy(it, group, source, k):
        return pltpu.make_async_remote_copy(
            src_ref=codes_out.at[it, group, lax.rem(spot + k, inner)],
            dst_ref=codes_in.at[it, group, source],
            send_sem=near_send.at[it, group, k], recv_sem=near_recv.at[it, group, source],
            device_id={"cell": near(k)}, device_id_type=MESH,
        )

    def step_copy(it, group, source, k):
        return pltpu.make_async_remote_copy(
            src_ref=steps_out.at[it, group, lax.rem(spot + k, inner)],
            dst_ref=steps_in.at[it, group, source],
            send_sem=step_send.at[it, group, k], recv_sem=step_recv.at[it, group, source],
            device_id={"cell": near(k)}, device_id_type=MESH,
        )

    def far_copy(it, source, k):
        return pltpu.make_async_remote_copy(
            src_ref=sums_own.at[it, lax.rem(here + k, outer)], dst_ref=sums_in.at[it, source],
            send_sem=far_send.at[it, k], recv_sem=far_recv.at[it, source],
            device_id={"cell": far(k)}, device_id_type=MESH,
        )

    def mid_copy(source, outward, along):
        target = lax.rem(here + outward, outer) * inner + lax.rem(spot + along, inner)
        return pltpu.make_async_remote_copy(
            src_ref=middle.at[source], dst_ref=middle.at[source],
            send_sem=mid_send.at[outward, along], recv_sem=mid_recv.at[source],
            device_id={"cell": target}, device_id_type=MESH,
        )

    def each_near(act):
        for k in range(1, inner):
            act(lax.rem(spot + inner - k, inner), k)

    def each_far(act):
        for k in range(1, outer):
            act(lax.rem(here + outer - k, outer), k)

    outwards = sorted(range(outer), key=lambda k: -min(k, outer - k))

    def each_mid(order, act):
        for outward in order:
            for along in range(inner):
                if outward + along > 0:
                    act(outward, along)

    def added(ref, count):
        total = ref[0]
        for c in range(1, count):
            total = total + ref[c]
        return total

    def loop(first, last, act):
        if last - first <= 4:
            for k in range(first, last):
                act(k)
        else:
            def body(k, _):
                act(k)
                return 0

            lax.fori_loop(first, last, body, 0)

    def part(r):
        return pl.ds(r * piece, piece)

    def place(r):
        for row in range(r * piece // side, (r + 1) * piece // side):
            for col in range(gene_blocks):
                dense[row * side : (row + 1) * side, col * side : (col + 1) * side] = held[
                    table[0, row * gene_blocks + col]
                ]

    def score(left, r, columns):
        return lax.dot_general(
            left, dense[part(r), columns], (((1,), (1,)), ((), ())),
            preferred_element_type=jnp.float32,
        )

    def iteration(it):
        if it == 0:
            with scope("place"):
                place(0)
            for r in range(parts):
                with scope("score"):
                    if r + 1 < parts:
                        place(r + 1)
                    mine[it, r] = score(first[...], r, slice(None))
                if r == 0:
                    with scope("barrier"):
                        pl.semaphore_wait(barrier, cells)
                pair_copy(it, r).start()
        else:
            order = outwards[::-1]
            for step, outward in enumerate(order):
                group = lax.rem(here + outward, outer)
                with scope("midwait"):
                    each_mid(
                        [outward],
                        lambda out, along: mid_copy(
                            group * inner + lax.rem(spot + along, inner), out, along
                        ).wait_recv(),
                    )
                left = jnp.concatenate(
                    [middle[group * inner + c] for c in range(inner)], axis=1
                )
                columns = pl.ds(pl.multiple_of(group * span, 128), span)
                with scope("score"):
                    for r in range(parts):
                        fresh = score(left, r, columns)
                        mine[it, r] = fresh if step == 0 else mine[it, r] + fresh
                        if step == outer - 1:
                            pair_copy(it, r).start()

        def merge(r):
            pair_copy(it, r).wait_recv()
            pieces = split_three(mine[it, r] + theirs[it, r])
            for i in range(it + 2):
                stacked[i * width : (i + 1) * width, part(r)] = pieces[i]

        with scope("merge"):
            for r in range(parts):
                merge(r)

        def product(columns):
            pair = jnp.dot(
                stacked[0 : 2 * width, :], columns, preferred_element_type=jnp.float32
            )
            return pair[:width] + pair[width:]

        def multiply(k):
            group = lax.rem(here + k, outer)
            wide = product(dense[:, pl.ds(pl.multiple_of(group * span, 128), span)])
            for c in range(inner):
                value = wide[:, c * chunk : (c + 1) * chunk]
                sums_near[group, c] = value
                coded, steps = encode(value)
                codes_out[it, group, c] = coded
                steps_out[it, group, c] = steps
            each_near(lambda _, k: near_copy(it, group, spot, k).start())
            each_near(lambda _, k: step_copy(it, group, spot, k).start())

        def gram():
            whole = stacked[0 : (it + 2) * width, :]
            cross = lax.dot_general(
                whole, whole, (((1,), (1,)), ((), ())), preferred_element_type=jnp.float32
            )
            cross = sum(cross[i * width : (i + 1) * width] for i in range(it + 2))
            total = sum(cross[:, i * width : (i + 1) * width] for i in range(it + 2))
            grams[it, spot] = jnp.concatenate([total[:half], total[half:]], axis=1)
            each_near(lambda _, k: gram_copy(it, spot, k).start())

        def forward(k):
            group = lax.rem(here + k, outer)
            each_near(lambda source, k: near_copy(it, group, source, k).wait_recv())
            each_near(lambda source, k: step_copy(it, group, source, k).wait_recv())
            total = sums_near[group, spot]
            for c in range(1, inner):
                source = lax.rem(spot + c, inner)
                total = total + decode(codes_in[it, group, source], steps_in[it, group, source])
            if isinstance(k, int) and k == 0:
                sums_in[it, here] = total
            else:
                sums_own[it, group] = total
                far_copy(it, here, k).start()

        with scope("gram"):
            pl.when(lead)(gram)
        with scope("multiply"):
            loop(1, outer + 1, multiply)

        @pl.when(lead)
        def _():
            with scope("gramwait"):
                each_near(lambda source, k: gram_copy(it, source, k).wait_recv())
            planes[it, here] = added(grams.at[it], inner)
            each_far(lambda _, k: plane_copy(it, here, k).start())

        with scope("forward"):
            loop(1, outer, forward)
            forward(0)

        @pl.when(lead)
        def _():
            with scope("planewait"):
                each_far(lambda source, k: plane_copy(it, source, k).wait_recv())
            totals[it] = added(planes.at[it], outer)
            total_copy(it).start()

        @pl.when(jnp.logical_not(lead))
        def _():
            with scope("totalwait"):
                total_copy(it).wait_recv()

        total = totals[it]
        total = jnp.concatenate([total[:, :width], total[:, width:]], axis=0)
        with scope("inverse"):
            inverse = inverse_factor(total)
        if it == 1:
            with scope("finish"):
                scale = jnp.sqrt(jnp.float32(cells * cell_dev))
                left = jnp.concatenate(
                    [jnp.concatenate([p] * 3, axis=1) for p in split_three(inverse)], axis=0
                )
                for r in range(parts):
                    final = jnp.dot(
                        left, stacked[:, part(r)], preferred_element_type=jnp.float32
                    )
                    final = final[:width] + final[width : 2 * width] + final[2 * width :]
                    basis_out[:, part(r)] = (final * scale).astype(basis_out.dtype)
        with scope("farwait"):
            each_far(lambda source, k: far_copy(it, source, k).wait_recv())
        with scope("result"):
            summed = added(sums_in.at[it], outer)
            result = jnp.dot(inverse, summed, precision=HIGH, preferred_element_type=jnp.float32)
            if it == 0:
                middle[cell] = result.astype(middle.dtype)
                each_mid(outwards, lambda out, along: mid_copy(cell, out, along).start())
            else:
                load_out[...] = result

    iteration(0)
    iteration(1)

    for it in range(2):
        for r in range(parts):
            pair_copy(it, r).wait_send()

        @pl.when(lead)
        def _():
            each_near(lambda _, k: gram_copy(it, spot, k).wait_send())
            each_far(lambda _, k: plane_copy(it, here, k).wait_send())
            total_copy(it).wait_send()

        loop(0, outer, lambda group: each_near(
            lambda _, k: near_copy(it, group, spot, k).wait_send()
        ))
        loop(0, outer, lambda group: each_near(
            lambda _, k: step_copy(it, group, spot, k).wait_send()
        ))
        each_far(lambda _, k: far_copy(it, here, k).wait_send())
    each_mid(outwards, lambda out, along: mid_copy(cell, out, along).wait_send())


def local(cells, genes, tiles, tile_row, tile_col, tile_count, start_basis):
    slots, side = tiles.shape[1], tiles.shape[-1]
    width, gene_dev = start_basis.shape
    gene_blocks = gene_dev // side
    cell_dev = ROW_BLOCKS * side
    chunk = gene_dev // cells
    parts = 2
    inner = 1
    while inner * inner * 4 <= cells and cells % (inner * 2) == 0:
        inner = inner * 2
    outer = cells // inner
    places = ROW_BLOCKS * gene_blocks
    dma = pltpu.SemaphoreType.DMA
    return pl.pallas_call(
        functools.partial(kernel, cells, inner, genes, parts),
        out_shape=(
            jax.ShapeDtypeStruct((width, cell_dev), jnp.bfloat16),
            jax.ShapeDtypeStruct((width, chunk), jnp.float32),
        ),
        in_specs=[
            pl.BlockSpec(memory_space=pltpu.SMEM),
            pl.BlockSpec(memory_space=pltpu.HBM),
            pl.BlockSpec(memory_space=pltpu.HBM),
            pl.BlockSpec(memory_space=pltpu.HBM),
            pl.BlockSpec(memory_space=pltpu.HBM),
        ],
        out_specs=(
            pl.BlockSpec(memory_space=pltpu.VMEM),
            pl.BlockSpec(memory_space=pltpu.VMEM),
        ),
        scratch_shapes=[
            pltpu.VMEM((1, slots), jnp.int32),
            pltpu.VMEM((1, slots), jnp.int32),
            pltpu.VMEM((1, places), jnp.int32),
            pltpu.SMEM((1, places), jnp.int32),
            pltpu.VMEM((slots + 1, side, side), jnp.bfloat16),
            pltpu.VMEM((cell_dev, gene_dev), jnp.bfloat16),
            pltpu.VMEM((width, gene_dev), jnp.bfloat16),
            pltpu.VMEM((2, parts, width, cell_dev // parts), jnp.float32),
            pltpu.VMEM((2, parts, width, cell_dev // parts), jnp.float32),
            pltpu.VMEM((3 * width, cell_dev), jnp.bfloat16),
            pltpu.VMEM((2, inner, width // 2, 2 * width), jnp.float32),
            pltpu.VMEM((2, outer, width // 2, 2 * width), jnp.float32),
            pltpu.VMEM((2, width // 2, 2 * width), jnp.float32),
            pltpu.VMEM((outer, inner, width, chunk), jnp.float32),
            pltpu.VMEM((2, outer, inner, width, chunk), jnp.int16),
            pltpu.VMEM((2, outer, inner, width, chunk), jnp.int16),
            pltpu.VMEM((2, outer, inner, 1, width), jnp.float32),
            pltpu.VMEM((2, outer, inner, 1, width), jnp.float32),
            pltpu.VMEM((2, outer, width, chunk), jnp.float32),
            pltpu.VMEM((2, outer, width, chunk), jnp.float32),
            pltpu.VMEM((cells, width, chunk), jnp.bfloat16),
            dma, dma((2,)), dma, dma,
            dma((2, parts)), dma((2, parts)),
            dma((2, inner)), dma((2, inner)), dma((2, outer)), dma((2, outer)), dma((2,)), dma((2,)),
            dma((2, outer, inner)), dma((2, outer, inner)),
            dma((2, outer, inner)), dma((2, outer, inner)), dma((2, outer)), dma((2, outer)),
            dma((outer, inner)), dma((cells,)),
        ],
        compiler_params=pltpu.CompilerParams(
            collective_id=0, has_side_effects=True, vmem_limit_bytes=36 * 1024 * 1024
        ),
    )(tile_count, *(
        pltpu.with_memory_space_constraint(array, pltpu.HBM)
        for array in (tile_row, tile_col, tiles[0], start_basis)
    ))


def solution(mesh):
    return jax.shard_map(
        functools.partial(local, mesh.shape["cell"], mesh.shape["gene"]),
        mesh=mesh,
        in_specs=(
            P("gene", "cell", None, None),
            P("gene", "cell"),
            P("gene", "cell"),
            P("gene", "cell"),
            P(None, "gene"),
        ),
        out_specs=(P(None, "cell"), P(None, ("gene", "cell"))),
        check_vma=False,
    )
```

```python
import functools

import jax
import jax.numpy as jnp
from jax import lax
from jax.experimental import pallas as pl
from jax.experimental.pallas import tpu as pltpu
from jax.sharding import PartitionSpec as P

ROW_BLOCKS = 8
PANEL = 4
LEVELS = 32766.0
MESH = pl.DeviceIdType.MESH
HIGH = lax.Precision.HIGHEST
scope = jax.named_scope


def split_three(value):
    high = value.astype(jnp.bfloat16)
    rest = value - high.astype(jnp.float32)
    middle = rest.astype(jnp.bfloat16)
    low = (rest - middle.astype(jnp.float32)).astype(jnp.bfloat16)
    return high, middle, low


def inverse_factor(gram):
    width = gram.shape[0]
    shape = (width, 2 * width)
    row = lax.broadcasted_iota(jnp.int32, shape, 0)
    lane = lax.broadcasted_iota(jnp.int32, shape, 1)
    both = jnp.concatenate([jnp.zeros_like(gram), gram], axis=1)
    both = jnp.where(row == lane, 1.0, both)
    pivots = jnp.ones(shape, jnp.float32)
    done = []
    start = 0

    def spread(first):
        return {
            j: jnp.broadcast_to(both[:, width + j : width + j + 1], both.shape)
            for j in range(first, min(first + PANEL, width))
        }

    ahead = spread(0)
    for first in range(0, width, PANEL):
        base = first // 8 * 8
        if base > start:
            done.append((both[: base - start], pivots[: base - start]))
            both = both[base - start :]
            pivots = pivots[base - start :]
            row = row[base - start :]
            ahead = {j: column[base - start :] for j, column in ahead.items()}
            start = base
        columns = ahead
        ahead = spread(first + PANEL)
        for j in range(first, first + PANEL):
            at = j - start
            column = columns.pop(j)
            pivot = column[at : at + 1]
            factor = jnp.where(row > j, column * (1.0 / pivot), 0.0)
            pivots = jnp.where(row == j, pivot, pivots)
            both = both - factor * both[at : at + 1]
            for later in (columns, ahead):
                for m in later:
                    later[m] = later[m] - factor * later[m][at : at + 1]
    done.append((both, pivots))
    both = jnp.concatenate([piece for piece, _ in done], axis=0)
    pivots = jnp.concatenate([piece for _, piece in done], axis=0)
    return (both * lax.rsqrt(pivots))[:, :width]


def diagonal(width):
    square = (width, width)
    return lax.broadcasted_iota(jnp.int32, square, 0) == lax.broadcasted_iota(jnp.int32, square, 1)


def encode(value):
    peak = jnp.max(jnp.abs(value), axis=1, keepdims=True)
    step = jnp.maximum(peak, 1e-30) * (1.0 / LEVELS)
    coded = jnp.round(value * (1.0 / step)).astype(jnp.int32).astype(jnp.int16)
    square = (value.shape[0], value.shape[0])
    turned = jnp.where(diagonal(square[0]), jnp.broadcast_to(step, square), 0.0)
    return coded, jnp.sum(turned, axis=0, keepdims=True)


def decode(coded, steps):
    square = (coded.shape[0], coded.shape[0])
    turned = jnp.where(diagonal(square[0]), jnp.broadcast_to(steps, square), 0.0)
    step = jnp.sum(turned, axis=1, keepdims=True)
    return coded.astype(jnp.int32).astype(jnp.float32) * step


def kernel(
    cells, inner, genes, parts,
    slot_count, slot_row, slot_col, tiles, start, basis_out, load_out,
    slots_in, places_out, table, held, dense, first, mine, theirs, stacked, grams, planes, factor,
    sums_near, codes_out, codes_in, steps_out, steps_in, sums_own, sums_in,
    columns, middle, load_res, load_in,
    tile_sem, slot_sem, table_sem, start_sem, pair_send, pair_recv,
    gram_send, gram_recv, plane_send, plane_recv, factor_send, factor_recv,
    near_send, near_recv, step_send, step_recv, far_send, far_recv,
    column_send, column_recv, mid_send, mid_recv, load_send, load_recv,
):
    cell = lax.axis_index("cell")
    gene = lax.axis_index("gene")
    slots, side, _ = tiles.shape
    width = start.shape[0]
    cell_dev, gene_dev = dense.shape
    gene_blocks = gene_dev // side
    chunk = gene_dev // cells
    piece = cell_dev // parts
    half = width // 2
    outer = cells // inner
    span = inner * chunk
    here = cell // inner
    spot = lax.rem(cell, inner)
    other = lax.rem(gene + 1, genes)
    head = genes - 1
    lead = gene == head
    follow = gene != head

    slot_copies = [
        pltpu.make_async_copy(slot_row, slots_in.at[0], slot_sem.at[0]),
        pltpu.make_async_copy(slot_col, slots_in.at[1], slot_sem.at[1]),
    ]
    for copy in slot_copies:
        copy.start()
    fetch = pltpu.make_async_copy(tiles, held.at[pl.ds(0, slots)], tile_sem)
    fetch.start()
    first_basis = pltpu.make_async_copy(start, first, start_sem)
    first_basis.start()

    def near(k):
        return here * inner + lax.rem(spot + k, inner)

    def far(k):
        return lax.rem(here + k, outer) * inner + spot

    barrier = pltpu.get_barrier_semaphore()
    greeted = 0
    for k in range(inner):
        for g in range(genes):
            if k + g > 0:
                pl.semaphore_signal(
                    barrier, inc=1,
                    device_id={"cell": near(k), "gene": lax.rem(gene + g, genes)},
                    device_id_type=MESH,
                )
                greeted += 1
    for k in range(1, outer):
        pl.semaphore_signal(barrier, inc=1, device_id={"cell": far(k)}, device_id_type=MESH)
        greeted += 1

    held[slots] = jnp.zeros((side, side), held.dtype)
    for copy in slot_copies:
        copy.wait()
    places = (cell_dev // side) * gene_blocks
    lane = lax.broadcasted_iota(jnp.int32, (1, slots), 1)
    spots = jnp.where(
        lane < slot_count[0, 0], slots_in[0] * gene_blocks + slots_in[1], places
    )
    square = (slots, slots)
    turned = jnp.where(diagonal(slots), jnp.broadcast_to(spots, square), 0)
    turned = jnp.sum(turned, axis=1, keepdims=True)
    flat = (slots, places)
    found = jnp.broadcast_to(turned, flat) == lax.broadcasted_iota(jnp.int32, flat, 1)
    found = jnp.where(found, lax.broadcasted_iota(jnp.int32, flat, 0), slots)
    places_out[...] = jnp.min(found, axis=0, keepdims=True)
    listing = pltpu.make_async_copy(places_out, table, table_sem)
    listing.start()
    listing.wait()
    fetch.wait()
    first_basis.wait()

    def remote(source, target, send_sem, recv_sem, **device):
        return pltpu.make_async_remote_copy(
            src_ref=source, dst_ref=target, send_sem=send_sem, recv_sem=recv_sem,
            device_id=device, device_id_type=MESH,
        )

    def pair_copy(it, r):
        return remote(
            mine.at[it, r], theirs.at[it, r], pair_send.at[0], pair_recv.at[it, r], gene=other
        )

    def gram_copy(it, k):
        return remote(
            grams.at[it, spot], grams.at[it, spot], gram_send.at[0], gram_recv.at[it],
            cell=near(k),
        )

    def plane_copy(it, k):
        return remote(
            planes.at[it, here], planes.at[it, here], plane_send.at[0], plane_recv.at[it],
            cell=far(k),
        )

    def near_copy(it, group, k):
        return remote(
            codes_out.at[it, group, k], codes_in.at[it, gene, group, k],
            near_send.at[0], near_recv.at[it, gene, group], cell=near(k), gene=head,
        )

    def step_copy(it, group, k):
        return remote(
            steps_out.at[it, group, k], steps_in.at[it, gene, group, k],
            step_send.at[0], step_recv.at[it, gene, group], cell=near(k), gene=head,
        )

    def far_copy(it, k):
        return remote(
            sums_own.at[it, lax.rem(here + k, outer)], sums_in.at[it, here],
            far_send.at[0], far_recv.at[it], cell=far(k),
        )

    def column_copy(target):
        return remote(
            columns.at[here], columns.at[here], column_send.at[0], column_recv.at[here],
            cell=target * inner + spot,
        )

    def mid_copy(group, g, k):
        return remote(
            columns.at[group, g], middle.at[group * inner + spot],
            mid_send.at[group], mid_recv.at[group], cell=near(k), gene=g,
        )

    def awaited(refs, sem):
        remote(refs, refs, pair_send.at[0], sem, gene=other).wait_recv()

    def drained(refs, sem):
        remote(refs, refs, sem, pair_recv.at[0, 0], gene=other).wait_send()

    def added(ref, count):
        total = ref[0]
        for c in range(1, count):
            total = total + ref[c]
        return total

    def loop(first, last, act):
        if last - first <= 4:
            for k in range(first, last):
                act(k)
        else:
            def body(k, _):
                act(k)
                return 0

            lax.fori_loop(first, last, body, 0)

    def part(r):
        return pl.ds(r * piece, piece)

    def along(m):
        return lax.rem(here + jnp.where(2 * here < outer, m, outer - m), outer)

    def place(r):
        for row in range(r * piece // side, (r + 1) * piece // side):
            for col in range(gene_blocks):
                dense[row * side : (row + 1) * side, col * side : (col + 1) * side] = held[
                    table[0, row * gene_blocks + col]
                ]

    def score(left, r, lanes):
        return lax.dot_general(
            left, dense[part(r), lanes], (((1,), (1,)), ((), ())),
            preferred_element_type=jnp.float32,
        )

    def first_scores():
        with scope("place"):
            place(0)
        for r in range(parts):
            with scope("score"):
                if r + 1 < parts:
                    place(r + 1)
                mine[0, r] = score(first[...], r, slice(None))
            if r == 0:
                with scope("barrier"):
                    pl.semaphore_wait(barrier, greeted)
            pair_copy(0, r).start()

    def second_scores():
        def step(m):
            group = along(m)
            with scope("midwait"):
                @pl.when(lead)
                def _():
                    awaited(middle.at[pl.ds(0, inner - 1)], mid_recv.at[group])
                    middle[group * inner + spot] = columns[group, head]

                @pl.when(follow)
                def _():
                    awaited(middle.at[pl.ds(0, inner)], mid_recv.at[group])

            left = jnp.concatenate([middle[group * inner + c] for c in range(inner)], axis=1)
            lanes = pl.ds(pl.multiple_of(group * span, 128), span)
            with scope("score"):
                for r in range(parts):
                    fresh = score(left, r, lanes)
                    if isinstance(m, int) and m == 0:
                        mine[1, r] = fresh
                    else:
                        mine[1, r] = mine[1, r] + fresh
                    if isinstance(m, int) and m == outer - 1:
                        pair_copy(1, r).start()

        step(0)
        loop(1, outer - 1, step)
        step(outer - 1)

    def share(group):
        for k in list(range(1, inner)) + [0]:
            for g in range(genes):
                if k > 0 or g != head:
                    mid_copy(group, g, k).start()

    def iteration(it):
        if it == 0:
            first_scores()
        else:
            second_scores()

        with scope("merge"):
            for r in range(parts):
                pair_copy(it, r).wait_recv()
                pieces = split_three(mine[it, r] + theirs[it, r])
                for i in range(it + 2):
                    stacked[i * width : (i + 1) * width, part(r)] = pieces[i]

        def gram():
            whole = stacked[0 : (it + 2) * width, :]
            cross = lax.dot_general(
                whole, whole, (((1,), (1,)), ((), ())), preferred_element_type=jnp.float32
            )
            cross = sum(cross[i * width : (i + 1) * width] for i in range(it + 2))
            total = sum(cross[:, i * width : (i + 1) * width] for i in range(it + 2))
            grams[it, spot] = jnp.concatenate([total[:half], total[half:]], axis=1)
            for k in range(1, inner):
                gram_copy(it, k).start()

        def multiply(m):
            group = lax.rem(here + m, outer)
            wide = jnp.dot(
                stacked[0 : 2 * width, :],
                dense[:, pl.ds(pl.multiple_of(group * span, 128), span)],
                preferred_element_type=jnp.float32,
            )
            wide = wide[:width] + wide[width:]
            for c in range(inner):
                sums_near[group, c] = wide[:, c * chunk : (c + 1) * chunk]
            for k in range(inner):
                coded, steps = encode(sums_near[group, lax.rem(spot + k, inner)])
                codes_out[it, group, k] = coded
                steps_out[it, group, k] = steps
            for k in range(1, inner):
                step_copy(it, group, k).start()
                near_copy(it, group, k).start()

            @pl.when(follow)
            def _():
                step_copy(it, group, 0).start()
                near_copy(it, group, 0).start()

        def forward(m):
            group = lax.rem(here + m, outer)
            own = isinstance(m, int) and m == 0
            for g in range(genes):
                low = 1 if g == head else 0
                awaited(steps_in.at[it, g, group, pl.ds(low, inner - low)], step_recv.at[it, g, group])
                awaited(codes_in.at[it, g, group, pl.ds(low, inner - low)], near_recv.at[it, g, group])
                total = sums_near[group, spot] if g == head else None
                for k in range(low, inner):
                    value = decode(codes_in[it, g, group, k], steps_in[it, g, group, k])
                    total = value if total is None else total + value
                if own:
                    sums_in[it, here, g] = total
                else:
                    sums_own[it, group, g] = total
            if not own:
                far_copy(it, m).start()

        def reduce():
            with scope("gramwait"):
                awaited(grams.at[it, pl.ds(0, inner - 1)], gram_recv.at[it])
            planes[it, here] = added(grams.at[it], inner)
            for k in range(1, outer):
                plane_copy(it, k).start()
            with scope("forward"):
                loop(1, outer, forward)
                forward(0)
            with scope("planewait"):
                awaited(planes.at[it, pl.ds(0, outer - 1)], plane_recv.at[it])
            total = added(planes.at[it], outer)
            total = jnp.concatenate([total[:, :width], total[:, width:]], axis=0)
            with scope("inverse"):
                inverse = inverse_factor(total)
            if it == 1:
                factor[...] = inverse
                remote(factor, factor, factor_send.at[0], factor_recv.at[0], gene=other).start()
            with scope("farwait"):
                awaited(sums_in.at[it, pl.ds(0, outer - 1)], far_recv.at[it])
            with scope("result"):
                summed = added(sums_in.at[it], outer)
                summed = jnp.concatenate([summed[g] for g in range(genes)], axis=1)
                result = jnp.dot(
                    inverse, summed, precision=HIGH, preferred_element_type=jnp.float32
                )
                result = [result[:, g * chunk : (g + 1) * chunk] for g in range(genes)]
                if it == 0:
                    for g in range(genes):
                        columns[here, g] = result[g].astype(columns.dtype)
                    for m in range(outer - 1, 0, -1):
                        column_copy(along(m)).start()
                    share(here)
                else:
                    load_res[...] = result[0]
                    remote(load_res, load_in, load_send.at[0], load_recv.at[0], gene=other).start()
                    load_out[...] = result[head]
            if it == 0:
                def relay(m):
                    group = along(m)
                    with scope("columnwait"):
                        awaited(columns.at[group], column_recv.at[group])
                    share(group)

                loop(1, outer, relay)

        with scope("gram"):
            pl.when(lead)(gram)
        with scope("multiply"):
            loop(1, outer + 1, multiply)
        pl.when(lead)(reduce)

    iteration(0)
    iteration(1)

    @pl.when(follow)
    def _():
        with scope("factorwait"):
            awaited(factor, factor_recv.at[0])

    with scope("finish"):
        scale = jnp.sqrt(jnp.float32(cells * cell_dev))
        left = jnp.concatenate(
            [jnp.concatenate([p] * 3, axis=1) for p in split_three(factor[...])], axis=0
        )
        for r in range(parts):
            final = jnp.dot(left, stacked[:, part(r)], preferred_element_type=jnp.float32)
            final = final[:width] + final[width : 2 * width] + final[2 * width :]
            basis_out[:, part(r)] = (final * scale).astype(basis_out.dtype)

    @pl.when(follow)
    def _():
        with scope("loadwait"):
            awaited(load_in, load_recv.at[0])
        load_out[...] = load_in[...]
        drained(codes_out, near_send.at[0])
        drained(steps_out, step_send.at[0])

    @pl.when(lead)
    def _():
        drained(codes_out.at[:, :, pl.ds(1, inner - 1)], near_send.at[0])
        drained(steps_out.at[:, :, pl.ds(1, inner - 1)], step_send.at[0])
        drained(grams.at[:, pl.ds(0, inner - 1)], gram_send.at[0])
        drained(planes.at[:, pl.ds(0, outer - 1)], plane_send.at[0])
        drained(sums_own.at[:, pl.ds(0, outer - 1)], far_send.at[0])
        drained(columns.at[pl.ds(0, outer - 1)], column_send.at[0])
        loop(0, outer, lambda group: drained(
            middle.at[pl.ds(0, inner * genes - 1)], mid_send.at[group]
        ))
        drained(factor, factor_send.at[0])
        drained(load_res, load_send.at[0])

    drained(mine, pair_send.at[0])


def local(cells, genes, tiles, tile_row, tile_col, tile_count, start_basis):
    slots, side = tiles.shape[1], tiles.shape[-1]
    width, gene_dev = start_basis.shape
    gene_blocks = gene_dev // side
    cell_dev = ROW_BLOCKS * side
    chunk = gene_dev // cells
    parts = 2
    inner = 1
    while inner * inner * 4 <= cells and cells % (inner * 2) == 0:
        inner = inner * 2
    outer = cells // inner
    places = ROW_BLOCKS * gene_blocks
    dma = pltpu.SemaphoreType.DMA
    return pl.pallas_call(
        functools.partial(kernel, cells, inner, genes, parts),
        out_shape=(
            jax.ShapeDtypeStruct((width, cell_dev), jnp.bfloat16),
            jax.ShapeDtypeStruct((width, chunk), jnp.float32),
        ),
        in_specs=[
            pl.BlockSpec(memory_space=pltpu.SMEM),
            pl.BlockSpec(memory_space=pltpu.HBM),
            pl.BlockSpec(memory_space=pltpu.HBM),
            pl.BlockSpec(memory_space=pltpu.HBM),
            pl.BlockSpec(memory_space=pltpu.HBM),
        ],
        out_specs=(
            pl.BlockSpec(memory_space=pltpu.VMEM),
            pl.BlockSpec(memory_space=pltpu.VMEM),
        ),
        scratch_shapes=[
            pltpu.VMEM((2, 1, slots), jnp.int32),
            pltpu.VMEM((1, places), jnp.int32),
            pltpu.SMEM((1, places), jnp.int32),
            pltpu.VMEM((slots + 1, side, side), jnp.bfloat16),
            pltpu.VMEM((cell_dev, gene_dev), jnp.bfloat16),
            pltpu.VMEM((width, gene_dev), jnp.bfloat16),
            pltpu.VMEM((2, parts, width, cell_dev // parts), jnp.float32),
            pltpu.VMEM((2, parts, width, cell_dev // parts), jnp.float32),
            pltpu.VMEM((3 * width, cell_dev), jnp.bfloat16),
            pltpu.VMEM((2, inner, width // 2, 2 * width), jnp.float32),
            pltpu.VMEM((2, outer, width // 2, 2 * width), jnp.float32),
            pltpu.VMEM((width, width), jnp.float32),
            pltpu.VMEM((outer, inner, width, chunk), jnp.float32),
            pltpu.VMEM((2, outer, inner, width, chunk), jnp.int16),
            pltpu.VMEM((2, genes, outer, inner, width, chunk), jnp.int16),
            pltpu.VMEM((2, outer, inner, 1, width), jnp.float32),
            pltpu.VMEM((2, genes, outer, inner, 1, width), jnp.float32),
            pltpu.VMEM((2, outer, genes, width, chunk), jnp.float32),
            pltpu.VMEM((2, outer, genes, width, chunk), jnp.float32),
            pltpu.VMEM((outer, genes, width, chunk), jnp.bfloat16),
            pltpu.VMEM((cells, width, chunk), jnp.bfloat16),
            pltpu.VMEM((width, chunk), jnp.float32),
            pltpu.VMEM((width, chunk), jnp.float32),
            dma, dma((2,)), dma, dma,
            dma((1,)), dma((2, parts)),
            dma((1,)), dma((2,)), dma((1,)), dma((2,)), dma((1,)), dma((1,)),
            dma((1,)), dma((2, genes, outer)), dma((1,)), dma((2, genes, outer)),
            dma((1,)), dma((2,)),
            dma((1,)), dma((outer,)), dma((outer,)), dma((outer,)), dma((1,)), dma((1,)),
        ],
        compiler_params=pltpu.CompilerParams(
            collective_id=0, has_side_effects=True, vmem_limit_bytes=44 * 1024 * 1024
        ),
    )(tile_count, *(
        pltpu.with_memory_space_constraint(array, pltpu.HBM)
        for array in (tile_row, tile_col, tiles[0], start_basis)
    ))


def solution(mesh):
    return jax.shard_map(
        functools.partial(local, mesh.shape["cell"], mesh.shape["gene"]),
        mesh=mesh,
        in_specs=(
            P("gene", "cell", None, None),
            P("gene", "cell"),
            P("gene", "cell"),
            P("gene", "cell"),
            P(None, "gene"),
        ),
        out_specs=(P(None, "cell"), P(None, ("gene", "cell"))),
        check_vma=False,
    )
```

```python
import functools

import jax
import jax.numpy as jnp
from jax import lax
from jax.experimental import pallas as pl
from jax.experimental.pallas import tpu as pltpu
from jax.sharding import PartitionSpec as P

ROW_BLOCKS = 8
PANEL = 4
LEVELS = 32766.0
MESH = pl.DeviceIdType.MESH
HIGH = lax.Precision.HIGHEST
scope = jax.named_scope


def split_three(value):
    high = value.astype(jnp.bfloat16)
    rest = value - high.astype(jnp.float32)
    middle = rest.astype(jnp.bfloat16)
    low = (rest - middle.astype(jnp.float32)).astype(jnp.bfloat16)
    return high, middle, low


def inverse_factor(gram):
    width = gram.shape[0]
    shape = (width, 2 * width)
    row = lax.broadcasted_iota(jnp.int32, shape, 0)
    lane = lax.broadcasted_iota(jnp.int32, shape, 1)
    both = jnp.concatenate([jnp.zeros_like(gram), gram], axis=1)
    both = jnp.where(row == lane, 1.0, both)
    pivots = jnp.ones(shape, jnp.float32)
    done = []
    start = 0

    def spread(first):
        return {
            j: jnp.broadcast_to(both[:, width + j : width + j + 1], both.shape)
            for j in range(first, min(first + PANEL, width))
        }

    ahead = spread(0)
    for first in range(0, width, PANEL):
        base = first // 8 * 8
        if base > start:
            done.append((both[: base - start], pivots[: base - start]))
            both = both[base - start :]
            pivots = pivots[base - start :]
            row = row[base - start :]
            ahead = {j: column[base - start :] for j, column in ahead.items()}
            start = base
        columns = ahead
        ahead = spread(first + PANEL)
        for j in range(first, first + PANEL):
            at = j - start
            column = columns.pop(j)
            pivot = column[at : at + 1]
            factor = jnp.where(row > j, column * (1.0 / pivot), 0.0)
            pivots = jnp.where(row == j, pivot, pivots)
            both = both - factor * both[at : at + 1]
            for later in (columns, ahead):
                for m in later:
                    later[m] = later[m] - factor * later[m][at : at + 1]
    done.append((both, pivots))
    both = jnp.concatenate([piece for piece, _ in done], axis=0)
    pivots = jnp.concatenate([piece for _, piece in done], axis=0)
    return (both * lax.rsqrt(pivots))[:, :width]


def diagonal(width):
    square = (width, width)
    return lax.broadcasted_iota(jnp.int32, square, 0) == lax.broadcasted_iota(jnp.int32, square, 1)


def turn(column):
    square = (column.shape[0], column.shape[0])
    turned = jnp.where(diagonal(square[0]), jnp.broadcast_to(column, square), 0.0)
    return jnp.sum(turned, axis=0, keepdims=True)


def turn_back(line, lanes):
    square = (line.shape[1], line.shape[1])
    turned = jnp.where(diagonal(square[0]), jnp.broadcast_to(line, square), 0.0)
    return jnp.broadcast_to(jnp.sum(turned, axis=1, keepdims=True), (square[0], lanes))


def encode(value):
    peak = jnp.max(jnp.abs(value), axis=0, keepdims=True)
    step = jnp.maximum(peak, 1e-30) * (1.0 / LEVELS)
    return jnp.round(value * (1.0 / step)).astype(jnp.int32).astype(jnp.int16), step


def decode(coded, step):
    return coded.astype(jnp.int32).astype(jnp.float32) * step


def kernel(
    cells, inner, genes, parts,
    slot_count, slot_row, slot_col, tiles, start, basis_out, load_out,
    slots_in, places_out, table, held, dense, first, mine, theirs, stacked, grams, planes, factor,
    sums_near, codes_out, codes_in, steps_out, steps_in, lines_out, lines_in, factors,
    sums_own, sums_in,
    columns, middle, load_res, load_in,
    tile_sem, slot_sem, table_sem, start_sem, pair_send, pair_recv,
    gram_send, gram_recv, plane_send, plane_recv, factor_send, factor_recv,
    near_send, near_recv, step_send, step_recv, line_send, line_recv, far_send, far_recv,
    column_send, column_recv, mid_send, mid_recv, load_send, load_recv,
):
    cell = lax.axis_index("cell")
    gene = lax.axis_index("gene")
    slots, side, _ = tiles.shape
    width = start.shape[0]
    cell_dev, gene_dev = dense.shape
    gene_blocks = gene_dev // side
    chunk = gene_dev // cells
    piece = cell_dev // parts
    half = width // 2
    outer = cells // inner
    span = inner * chunk
    here = cell // inner
    spot = lax.rem(cell, inner)
    other = lax.rem(gene + 1, genes)
    head = genes - 1
    lead = gene == head
    follow = gene != head

    slot_copies = [
        pltpu.make_async_copy(slot_row, slots_in.at[0], slot_sem.at[0]),
        pltpu.make_async_copy(slot_col, slots_in.at[1], slot_sem.at[1]),
    ]
    for copy in slot_copies:
        copy.start()
    fetch = pltpu.make_async_copy(tiles, held.at[pl.ds(0, slots)], tile_sem)
    fetch.start()
    first_basis = pltpu.make_async_copy(start, first, start_sem)
    first_basis.start()

    def near(k):
        return here * inner + lax.rem(spot + k, inner)

    def far(k):
        return lax.rem(here + k, outer) * inner + spot

    barrier = pltpu.get_barrier_semaphore()
    greeted = 0
    for k in range(inner):
        for g in range(genes):
            if k + g > 0:
                pl.semaphore_signal(
                    barrier, inc=1,
                    device_id={"cell": near(k), "gene": lax.rem(gene + g, genes)},
                    device_id_type=MESH,
                )
                greeted += 1
    for k in range(1, outer):
        pl.semaphore_signal(barrier, inc=1, device_id={"cell": far(k)}, device_id_type=MESH)
        greeted += 1

    held[slots] = jnp.zeros((side, side), held.dtype)
    for copy in slot_copies:
        copy.wait()
    places = (cell_dev // side) * gene_blocks
    lane = lax.broadcasted_iota(jnp.int32, (1, slots), 1)
    spots = jnp.where(
        lane < slot_count[0, 0], slots_in[0] * gene_blocks + slots_in[1], places
    )
    square = (slots, slots)
    turned = jnp.where(diagonal(slots), jnp.broadcast_to(spots, square), 0)
    turned = jnp.sum(turned, axis=1, keepdims=True)
    flat = (slots, places)
    found = jnp.broadcast_to(turned, flat) == lax.broadcasted_iota(jnp.int32, flat, 1)
    found = jnp.where(found, lax.broadcasted_iota(jnp.int32, flat, 0), slots)
    places_out[...] = jnp.min(found, axis=0, keepdims=True)
    listing = pltpu.make_async_copy(places_out, table, table_sem)
    listing.start()
    listing.wait()
    fetch.wait()
    first_basis.wait()

    def remote(source, target, send_sem, recv_sem, **device):
        return pltpu.make_async_remote_copy(
            src_ref=source, dst_ref=target, send_sem=send_sem, recv_sem=recv_sem,
            device_id=device, device_id_type=MESH,
        )

    def pair_copy(it, r):
        return remote(
            mine.at[it, r], theirs.at[it, r], pair_send.at[0], pair_recv.at[it, r], gene=other
        )

    def gram_copy(it, k):
        return remote(
            grams.at[it, spot], grams.at[it, spot], gram_send.at[0], gram_recv.at[it],
            cell=near(k),
        )

    def plane_copy(it, k):
        return remote(
            planes.at[it, here], planes.at[it, here], plane_send.at[0], plane_recv.at[it],
            cell=far(k),
        )

    def near_copy(it, group, k):
        return remote(
            codes_out.at[it, group, k], codes_in.at[it, gene, group, k],
            near_send.at[0], near_recv.at[it, gene, group], cell=near(k), gene=head,
        )

    def step_copy(it, group, k):
        return remote(
            steps_out.at[it, group, k], steps_in.at[it, gene, group, k],
            step_send.at[0], step_recv.at[it, gene, group], cell=near(k), gene=head,
        )

    def line_copy(it, k):
        return remote(
            lines_out.at[it], lines_in.at[it, gene, k],
            line_send.at[0], line_recv.at[it, gene], cell=near(k), gene=head,
        )

    def far_copy(it, group):
        return remote(
            sums_own.at[it, group], sums_in.at[it, here],
            far_send.at[0], far_recv.at[it], cell=group * inner + spot,
        )

    def column_copy(target):
        return remote(
            columns.at[here], columns.at[here], column_send.at[0], column_recv.at[here],
            cell=target * inner + spot,
        )

    def mid_copy(group, g, k):
        return remote(
            columns.at[group, g], middle.at[group * inner + spot],
            mid_send.at[group], mid_recv.at[group], cell=near(k), gene=g,
        )

    def awaited(refs, sem):
        remote(refs, refs, pair_send.at[0], sem, gene=other).wait_recv()

    def drained(refs, sem):
        remote(refs, refs, sem, pair_recv.at[0, 0], gene=other).wait_send()

    def added(ref, count):
        total = ref[0]
        for c in range(1, count):
            total = total + ref[c]
        return total

    def loop(first, last, act):
        if last - first <= 4:
            for k in range(first, last):
                act(k)
        else:
            def body(k, _):
                act(k)
                return 0

            lax.fori_loop(first, last, body, 0)

    def part(r):
        return pl.ds(r * piece, piece)

    def along(m):
        return lax.rem(here + jnp.where(2 * here < outer, m, outer - m), outer)

    def place(low, high):
        for row in range(cell_dev // side):
            for col in range(low, high):
                dense[row * side : (row + 1) * side, col * side : (col + 1) * side] = held[
                    table[0, row * gene_blocks + col]
                ]

    def score(left, r, lanes):
        return lax.dot_general(
            left, dense[part(r), lanes], (((1,), (1,)), ((), ())),
            preferred_element_type=jnp.float32,
        )

    def first_scores():
        stages = 4
        share_cols = gene_blocks // stages
        with scope("place"):
            place(0, share_cols)
        for q in range(stages):
            lanes = slice(q * share_cols * side, (q + 1) * share_cols * side)
            with scope("score"):
                if q + 1 < stages:
                    place((q + 1) * share_cols, (q + 2) * share_cols)
                for r in range(parts):
                    fresh = score(first[:, lanes], r, lanes)
                    mine[0, r] = fresh if q == 0 else mine[0, r] + fresh
                    if q == stages - 1:
                        if r == 0:
                            pl.semaphore_wait(barrier, greeted)
                        pair_copy(0, r).start()

    def second_scores():
        def step(m):
            group = along(m)
            with scope("midwait"):
                @pl.when(lead)
                def _():
                    awaited(middle.at[pl.ds(0, inner - 1)], mid_recv.at[group])
                    middle[group * inner + spot] = columns[group, head]

                @pl.when(follow)
                def _():
                    awaited(middle.at[pl.ds(0, inner)], mid_recv.at[group])

            left = jnp.concatenate([middle[group * inner + c] for c in range(inner)], axis=1)
            lanes = pl.ds(pl.multiple_of(group * span, 128), span)
            with scope("score"):
                for r in range(parts):
                    fresh = score(left, r, lanes)
                    if isinstance(m, int) and m == 0:
                        mine[1, r] = fresh
                    else:
                        mine[1, r] = mine[1, r] + fresh
                    if isinstance(m, int) and m == outer - 1:
                        pair_copy(1, r).start()

        step(0)
        loop(1, outer - 1, step)
        step(outer - 1)

    def share(group):
        for k in list(range(1, inner)) + [0]:
            for g in range(genes):
                if k > 0 or g != head:
                    mid_copy(group, g, k).start()

    def iteration(it):
        if it == 0:
            first_scores()
        else:
            second_scores()

        with scope("merge"):
            peak = None
            for r in range(parts):
                pair_copy(it, r).wait_recv()
                whole = mine[it, r] + theirs[it, r]
                most = jnp.max(jnp.abs(whole), axis=1, keepdims=True)
                peak = most if peak is None else jnp.maximum(peak, most)
                pieces = split_three(whole)
                for i in range(it + 2):
                    stacked[i * width : (i + 1) * width, part(r)] = pieces[i]

            peak = jnp.maximum(peak, 1e-30)
            lines_out[it] = turn(peak)
            shrink = jnp.broadcast_to(1.0 / peak, (width, chunk))
            for k in range(1, inner):
                line_copy(it, k).start()

            @pl.when(follow)
            def _():
                line_copy(it, 0).start()

        def gram():
            whole = stacked[0 : (it + 2) * width, :]
            cross = lax.dot_general(
                whole, whole, (((1,), (1,)), ((), ())), preferred_element_type=jnp.float32
            )
            cross = sum(cross[i * width : (i + 1) * width] for i in range(it + 2))
            total = sum(cross[:, i * width : (i + 1) * width] for i in range(it + 2))
            grams[it, spot] = jnp.concatenate([total[:half], total[half:]], axis=1)
            for k in range(1, inner):
                gram_copy(it, k).start()

        def multiply(m):
            group = along(outer - m)
            wide = jnp.dot(
                stacked[0 : 2 * width, :],
                dense[:, pl.ds(pl.multiple_of(group * span, 128), span)],
                preferred_element_type=jnp.float32,
            )
            wide = wide[:width] + wide[width:]
            for c in range(inner):
                sums_near[group, c] = wide[:, c * chunk : (c + 1) * chunk]
            for k in range(inner):
                coded, steps = encode(sums_near[group, lax.rem(spot + k, inner)] * shrink)
                codes_out[it, group, k] = coded
                steps_out[it, group, k] = steps
            for k in range(1, inner):
                step_copy(it, group, k).start()
                near_copy(it, group, k).start()

            @pl.when(follow)
            def _():
                step_copy(it, group, 0).start()
                near_copy(it, group, 0).start()

        def forward(m):
            group = along(outer - m)
            own = isinstance(m, int) and m == outer
            for g in range(genes):
                low = 1 if g == head else 0
                awaited(steps_in.at[it, g, group, pl.ds(low, inner - low)], step_recv.at[it, g, group])
                awaited(codes_in.at[it, g, group, pl.ds(low, inner - low)], near_recv.at[it, g, group])
                total = sums_near[group, spot] if g == head else None
                for k in range(low, inner):
                    value = decode(codes_in[it, g, group, k], steps_in[it, g, group, k]) * factors[g, k]
                    total = value if total is None else total + value
                if own:
                    sums_in[it, here, g] = total
                else:
                    sums_own[it, group, g] = total
            if not own:
                far_copy(it, group).start()

        def reduce():
            with scope("gramwait"):
                awaited(grams.at[it, pl.ds(0, inner - 1)], gram_recv.at[it])
            planes[it, here] = added(grams.at[it], inner)
            for k in range(1, outer):
                plane_copy(it, k).start()
            with scope("forward"):
                for g in range(genes):
                    low = 1 if g == head else 0
                    awaited(lines_in.at[it, g, pl.ds(low, inner - low)], line_recv.at[it, g])
                    for k in range(low, inner):
                        factors[g, k] = turn_back(lines_in[it, g, k], chunk)
                loop(1, outer, forward)
                forward(outer)
            with scope("planewait"):
                awaited(planes.at[it, pl.ds(0, outer - 1)], plane_recv.at[it])
            total = added(planes.at[it], outer)
            total = jnp.concatenate([total[:, :width], total[:, width:]], axis=0)
            with scope("inverse"):
                inverse = inverse_factor(total)
            if it == 1:
                factor[...] = inverse
                remote(factor, factor, factor_send.at[0], factor_recv.at[0], gene=other).start()
            with scope("farwait"):
                awaited(sums_in.at[it, pl.ds(0, outer - 1)], far_recv.at[it])
            with scope("result"):
                summed = added(sums_in.at[it], outer)
                summed = jnp.concatenate([summed[g] for g in range(genes)], axis=1)
                result = jnp.dot(
                    inverse, summed, precision=HIGH, preferred_element_type=jnp.float32
                )
                result = [result[:, g * chunk : (g + 1) * chunk] for g in range(genes)]
                if it == 0:
                    for g in range(genes):
                        columns[here, g] = result[g].astype(columns.dtype)
                    for m in range(outer - 1, 0, -1):
                        column_copy(along(m)).start()
                    share(here)
                else:
                    load_res[...] = result[0]
                    remote(load_res, load_in, load_send.at[0], load_recv.at[0], gene=other).start()
                    load_out[...] = result[head]
            if it == 0:
                def relay(m):
                    group = along(m)
                    with scope("columnwait"):
                        awaited(columns.at[group], column_recv.at[group])
                    share(group)

                loop(1, outer, relay)

        with scope("gram"):
            pl.when(lead)(gram)
        with scope("multiply"):
            loop(1, outer + 1, multiply)
        pl.when(lead)(reduce)

    iteration(0)
    iteration(1)

    @pl.when(follow)
    def _():
        with scope("factorwait"):
            awaited(factor, factor_recv.at[0])

    with scope("finish"):
        scale = jnp.sqrt(jnp.float32(cells * cell_dev))
        left = jnp.concatenate(
            [jnp.concatenate([p] * 3, axis=1) for p in split_three(factor[...])], axis=0
        )
        for r in range(parts):
            final = jnp.dot(left, stacked[:, part(r)], preferred_element_type=jnp.float32)
            final = final[:width] + final[width : 2 * width] + final[2 * width :]
            basis_out[:, part(r)] = (final * scale).astype(basis_out.dtype)

    @pl.when(follow)
    def _():
        with scope("loadwait"):
            awaited(load_in, load_recv.at[0])
        load_out[...] = load_in[...]
        drained(codes_out, near_send.at[0])
        drained(steps_out, step_send.at[0])
        drained(lines_in.at[:, 0], line_send.at[0])

    @pl.when(lead)
    def _():
        drained(codes_out.at[:, :, pl.ds(1, inner - 1)], near_send.at[0])
        drained(steps_out.at[:, :, pl.ds(1, inner - 1)], step_send.at[0])
        drained(grams.at[:, pl.ds(0, inner - 1)], gram_send.at[0])
        drained(lines_in.at[:, 0, pl.ds(1, inner - 1)], line_send.at[0])
        drained(planes.at[:, pl.ds(0, outer - 1)], plane_send.at[0])
        drained(sums_own.at[:, pl.ds(0, outer - 1)], far_send.at[0])
        drained(columns.at[pl.ds(0, outer - 1)], column_send.at[0])
        loop(0, outer, lambda group: drained(
            middle.at[pl.ds(0, inner * genes - 1)], mid_send.at[group]
        ))
        drained(factor, factor_send.at[0])
        drained(load_res, load_send.at[0])

    drained(mine, pair_send.at[0])


def local(cells, genes, tiles, tile_row, tile_col, tile_count, start_basis):
    slots, side = tiles.shape[1], tiles.shape[-1]
    width, gene_dev = start_basis.shape
    gene_blocks = gene_dev // side
    cell_dev = ROW_BLOCKS * side
    chunk = gene_dev // cells
    parts = 2
    inner = 1
    while inner * inner * 4 <= cells and cells % (inner * 2) == 0:
        inner = inner * 2
    outer = cells // inner
    places = ROW_BLOCKS * gene_blocks
    dma = pltpu.SemaphoreType.DMA
    shapes = (
        jax.ShapeDtypeStruct((width, cell_dev), jnp.bfloat16),
        jax.ShapeDtypeStruct((width, chunk), jnp.float32),
    )
    results = pl.pallas_call(
        functools.partial(kernel, cells, inner, genes, parts),
        out_shape=shapes,
        in_specs=[
            pl.BlockSpec(memory_space=pltpu.SMEM),
            pl.BlockSpec(memory_space=pltpu.HBM),
            pl.BlockSpec(memory_space=pltpu.HBM),
            pl.BlockSpec(memory_space=pltpu.HBM),
            pl.BlockSpec(memory_space=pltpu.HBM),
        ],
        out_specs=(
            pl.BlockSpec(memory_space=pltpu.VMEM),
            pl.BlockSpec(memory_space=pltpu.VMEM),
        ),
        scratch_shapes=[
            pltpu.VMEM((2, 1, slots), jnp.int32),
            pltpu.VMEM((1, places), jnp.int32),
            pltpu.SMEM((1, places), jnp.int32),
            pltpu.VMEM((slots + 1, side, side), jnp.bfloat16),
            pltpu.VMEM((cell_dev, gene_dev), jnp.bfloat16),
            pltpu.VMEM((width, gene_dev), jnp.bfloat16),
            pltpu.VMEM((2, parts, width, cell_dev // parts), jnp.float32),
            pltpu.VMEM((2, parts, width, cell_dev // parts), jnp.float32),
            pltpu.VMEM((3 * width, cell_dev), jnp.bfloat16),
            pltpu.VMEM((2, inner, width // 2, 2 * width), jnp.float32),
            pltpu.VMEM((2, outer, width // 2, 2 * width), jnp.float32),
            pltpu.VMEM((width, width), jnp.float32),
            pltpu.VMEM((outer, inner, width, chunk), jnp.float32),
            pltpu.VMEM((2, outer, inner, width, chunk), jnp.int16),
            pltpu.VMEM((2, genes, outer, inner, width, chunk), jnp.int16),
            pltpu.VMEM((2, outer, inner, 1, chunk), jnp.float32),
            pltpu.VMEM((2, genes, outer, inner, 1, chunk), jnp.float32),
            pltpu.VMEM((2, 1, width), jnp.float32),
            pltpu.VMEM((2, genes, inner, 1, width), jnp.float32),
            pltpu.VMEM((genes, inner, width, chunk), jnp.float32),
            pltpu.VMEM((2, outer, genes, width, chunk), jnp.float32),
            pltpu.VMEM((2, outer, genes, width, chunk), jnp.float32),
            pltpu.VMEM((outer, genes, width, chunk), jnp.bfloat16),
            pltpu.VMEM((cells, width, chunk), jnp.bfloat16),
            pltpu.VMEM((width, chunk), jnp.float32),
            pltpu.VMEM((width, chunk), jnp.float32),
            dma, dma((2,)), dma, dma,
            dma((1,)), dma((2, parts)),
            dma((1,)), dma((2,)), dma((1,)), dma((2,)), dma((1,)), dma((1,)),
            dma((1,)), dma((2, genes, outer)), dma((1,)), dma((2, genes, outer)),
            dma((1,)), dma((2, genes)), dma((1,)), dma((2,)),
            dma((1,)), dma((outer,)), dma((outer,)), dma((outer,)), dma((1,)), dma((1,)),
        ],
        compiler_params=pltpu.CompilerParams(
            collective_id=0, has_side_effects=True, vmem_limit_bytes=44 * 1024 * 1024
        ),
    )(tile_count, *(
        pltpu.with_memory_space_constraint(array, pltpu.HBM)
        for array in (tile_row, tile_col, tiles[0], start_basis)
    ))
    return pl.pallas_call(
        deliver,
        out_shape=shapes,
        in_specs=[pl.BlockSpec(memory_space=pltpu.VMEM)] * 2,
        out_specs=(pl.BlockSpec(memory_space=pl.ANY),) * 2,
        scratch_shapes=[dma((2,))],
        compiler_params=pltpu.CompilerParams(vmem_limit_bytes=1024 * 1024),
    )(*results)


def deliver(basis, load, basis_out, load_out, sems):
    copies = [
        pltpu.make_async_copy(basis, basis_out, sems.at[0]),
        pltpu.make_async_copy(load, load_out, sems.at[1]),
    ]
    for copy in copies:
        copy.start()
    for copy in copies:
        copy.wait()


def solution(mesh):
    return jax.shard_map(
        functools.partial(local, mesh.shape["cell"], mesh.shape["gene"]),
        mesh=mesh,
        in_specs=(
            P("gene", "cell", None, None),
            P("gene", "cell"),
            P("gene", "cell"),
            P("gene", "cell"),
            P(None, "gene"),
        ),
        out_specs=(P(None, "cell"), P(None, ("gene", "cell"))),
        check_vma=False,
    )
```

```python
import functools

import jax
import jax.numpy as jnp
from jax import lax
from jax.experimental import pallas as pl
from jax.experimental.pallas import tpu as pltpu
from jax.sharding import PartitionSpec as P

ROW_BLOCKS = 8
PANEL = 4
LEVELS = 32766.0
MESH = pl.DeviceIdType.MESH
HIGH = lax.Precision.HIGHEST
scope = jax.named_scope


def split_three(value):
    high = value.astype(jnp.bfloat16)
    rest = value - high.astype(jnp.float32)
    middle = rest.astype(jnp.bfloat16)
    low = (rest - middle.astype(jnp.float32)).astype(jnp.bfloat16)
    return high, middle, low


def inverse_factor(gram):
    width = gram.shape[0]
    shape = (width, 2 * width)
    row = lax.broadcasted_iota(jnp.int32, shape, 0)
    lane = lax.broadcasted_iota(jnp.int32, shape, 1)
    both = jnp.concatenate([jnp.zeros_like(gram), gram], axis=1)
    both = jnp.where(row == lane, 1.0, both)
    pivots = jnp.ones(shape, jnp.float32)
    done = []
    start = 0

    def spread(first):
        return {
            j: jnp.broadcast_to(both[:, width + j : width + j + 1], both.shape)
            for j in range(first, min(first + PANEL, width))
        }

    ahead = spread(0)
    for first in range(0, width, PANEL):
        base = first // 8 * 8
        if base > start:
            done.append((both[: base - start], pivots[: base - start]))
            both = both[base - start :]
            pivots = pivots[base - start :]
            row = row[base - start :]
            ahead = {j: column[base - start :] for j, column in ahead.items()}
            start = base
        columns = ahead
        ahead = spread(first + PANEL)
        for j in range(first, first + PANEL):
            at = j - start
            column = columns.pop(j)
            pivot = column[at : at + 1]
            factor = jnp.where(row > j, column * (1.0 / pivot), 0.0)
            pivots = jnp.where(row == j, pivot, pivots)
            both = both - factor * both[at : at + 1]
            for later in (columns, ahead):
                for m in later:
                    later[m] = later[m] - factor * later[m][at : at + 1]
    done.append((both, pivots))
    both = jnp.concatenate([piece for piece, _ in done], axis=0)
    pivots = jnp.concatenate([piece for _, piece in done], axis=0)
    return (both * lax.rsqrt(pivots))[:, :width]


def diagonal(width):
    square = (width, width)
    return lax.broadcasted_iota(jnp.int32, square, 0) == lax.broadcasted_iota(jnp.int32, square, 1)


def turn(column):
    square = (column.shape[0], column.shape[0])
    turned = jnp.where(diagonal(square[0]), jnp.broadcast_to(column, square), 0.0)
    return jnp.sum(turned, axis=0, keepdims=True)


def turn_back(line, lanes):
    square = (line.shape[1], line.shape[1])
    turned = jnp.where(diagonal(square[0]), jnp.broadcast_to(line, square), 0.0)
    return jnp.broadcast_to(jnp.sum(turned, axis=1, keepdims=True), (square[0], lanes))


def encode(value):
    peak = jnp.max(jnp.abs(value), axis=0, keepdims=True)
    step = jnp.maximum(peak, 1e-30) * (1.0 / LEVELS)
    return jnp.round(value * (1.0 / step)).astype(jnp.int32).astype(jnp.int16), step


def decode(coded, step):
    return coded.astype(jnp.int32).astype(jnp.float32) * step


def kernel(
    cells, inner, genes, parts,
    slot_count, slot_row, slot_col, tiles, start, basis_out, load_out,
    slots_in, places_out, table, held, dense, first, mine, theirs, stacked, grams, planes, factor,
    sums_near, codes_out, codes_in, steps_out, steps_in, lines_out, lines_in, factors,
    sums_own, far_out, far_in, fars_out, fars_in, tails_out, tails_in, gains, stretch,
    columns, middle, load_res, load_in,
    tile_sem, slot_sem, table_sem, start_sem, pair_send, pair_recv,
    gram_send, gram_recv, plane_send, plane_recv, factor_send, factor_recv,
    near_send, near_recv, step_send, step_recv, line_send, line_recv,
    far_send, far_recv, fars_send, fars_recv, tail_send, tail_recv,
    column_send, column_recv, mid_send, mid_recv, load_send, load_recv,
):
    cell = lax.axis_index("cell")
    gene = lax.axis_index("gene")
    slots, side, _ = tiles.shape
    width = start.shape[0]
    cell_dev, gene_dev = dense.shape
    gene_blocks = gene_dev // side
    chunk = gene_dev // cells
    piece = cell_dev // parts
    half = width // 2
    outer = cells // inner
    span = inner * chunk
    here = cell // inner
    spot = lax.rem(cell, inner)
    other = lax.rem(gene + 1, genes)
    head = genes - 1
    lead = gene == head
    follow = gene != head

    slot_copies = [
        pltpu.make_async_copy(slot_row, slots_in.at[0], slot_sem.at[0]),
        pltpu.make_async_copy(slot_col, slots_in.at[1], slot_sem.at[1]),
    ]
    for copy in slot_copies:
        copy.start()
    fetch = pltpu.make_async_copy(tiles, held.at[pl.ds(0, slots)], tile_sem)
    fetch.start()
    first_basis = pltpu.make_async_copy(start, first, start_sem)
    first_basis.start()

    def near(k):
        return here * inner + lax.rem(spot + k, inner)

    def far(k):
        return lax.rem(here + k, outer) * inner + spot

    barrier = pltpu.get_barrier_semaphore()
    greeted = 0
    for k in range(inner):
        for g in range(genes):
            if k + g > 0:
                pl.semaphore_signal(
                    barrier, inc=1,
                    device_id={"cell": near(k), "gene": lax.rem(gene + g, genes)},
                    device_id_type=MESH,
                )
                greeted += 1
    for k in range(1, outer):
        pl.semaphore_signal(barrier, inc=1, device_id={"cell": far(k)}, device_id_type=MESH)
        greeted += 1

    held[slots] = jnp.zeros((side, side), held.dtype)
    for copy in slot_copies:
        copy.wait()
    places = (cell_dev // side) * gene_blocks
    lane = lax.broadcasted_iota(jnp.int32, (1, slots), 1)
    spots = jnp.where(
        lane < slot_count[0, 0], slots_in[0] * gene_blocks + slots_in[1], places
    )
    square = (slots, slots)
    turned = jnp.where(diagonal(slots), jnp.broadcast_to(spots, square), 0)
    turned = jnp.sum(turned, axis=1, keepdims=True)
    flat = (slots, places)
    found = jnp.broadcast_to(turned, flat) == lax.broadcasted_iota(jnp.int32, flat, 1)
    found = jnp.where(found, lax.broadcasted_iota(jnp.int32, flat, 0), slots)
    places_out[...] = jnp.min(found, axis=0, keepdims=True)
    listing = pltpu.make_async_copy(places_out, table, table_sem)
    listing.start()
    listing.wait()
    fetch.wait()
    first_basis.wait()

    def remote(source, target, send_sem, recv_sem, **device):
        return pltpu.make_async_remote_copy(
            src_ref=source, dst_ref=target, send_sem=send_sem, recv_sem=recv_sem,
            device_id=device, device_id_type=MESH,
        )

    def pair_copy(it, r):
        return remote(
            mine.at[it, r], theirs.at[it, r], pair_send.at[0], pair_recv.at[it, r], gene=other
        )

    def gram_copy(it, k):
        return remote(
            grams.at[it, spot], grams.at[it, spot], gram_send.at[0], gram_recv.at[it],
            cell=near(k), gene=head,
        )

    def plane_copy(it, k):
        return remote(
            planes.at[it, here], planes.at[it, here], plane_send.at[0], plane_recv.at[it],
            cell=far(k),
        )

    def near_copy(it, group, k):
        return remote(
            codes_out.at[it, group, k], codes_in.at[it, gene, group, k],
            near_send.at[0], near_recv.at[gene, group], cell=near(k), gene=head,
        )

    def step_copy(it, group, k):
        return remote(
            steps_out.at[it, group, k], steps_in.at[it, gene, group, k],
            step_send.at[0], step_recv.at[gene, group], cell=near(k), gene=head,
        )

    def line_copy(it, k):
        return remote(
            lines_out.at[it], lines_in.at[it, gene, k],
            line_send.at[0], line_recv.at[it, gene], cell=near(k), gene=head,
        )

    def far_copy(it, group):
        return remote(
            far_out.at[it, group], far_in.at[it, here],
            far_send.at[0], far_recv.at[it], cell=group * inner + spot,
        )

    def fars_copy(it, group):
        return remote(
            fars_out.at[it, group], fars_in.at[it, here],
            fars_send.at[0], fars_recv.at[it], cell=group * inner + spot,
        )

    def tail_copy(it, k):
        return remote(
            tails_out.at[it], tails_in.at[it, here],
            tail_send.at[0], tail_recv.at[it], cell=far(k),
        )

    def column_copy(target):
        return remote(
            columns.at[here], columns.at[here], column_send.at[0], column_recv.at[here],
            cell=target * inner + spot,
        )

    def mid_copy(group, g, k):
        return remote(
            columns.at[group, g], middle.at[group * inner + spot],
            mid_send.at[group], mid_recv.at[group], cell=near(k), gene=g,
        )

    def awaited(refs, sem):
        remote(refs, refs, pair_send.at[0], sem, gene=other).wait_recv()

    def drained(refs, sem):
        remote(refs, refs, sem, pair_recv.at[0, 0], gene=other).wait_send()

    def added(ref, count):
        total = ref[0]
        for c in range(1, count):
            total = total + ref[c]
        return total

    def loop(first, last, act):
        if last - first <= 4:
            for k in range(first, last):
                act(k)
        else:
            def body(k, _):
                act(k)
                return 0

            lax.fori_loop(first, last, body, 0)

    def part(r):
        return pl.ds(r * piece, piece)

    def along(m):
        return lax.rem(here + jnp.where(2 * here < outer, m, outer - m), outer)

    def place(low, high):
        for row in range(cell_dev // side):
            for col in range(low, high):
                dense[row * side : (row + 1) * side, col * side : (col + 1) * side] = held[
                    table[0, row * gene_blocks + col]
                ]

    def score(left, r, lanes):
        return lax.dot_general(
            left, dense[part(r), lanes], (((1,), (1,)), ((), ())),
            preferred_element_type=jnp.float32,
        )

    def first_scores():
        stages = 4
        share_cols = gene_blocks // stages
        with scope("place"):
            place(0, share_cols)
        for q in range(stages):
            lanes = slice(q * share_cols * side, (q + 1) * share_cols * side)
            with scope("score"):
                if q + 1 < stages:
                    place((q + 1) * share_cols, (q + 2) * share_cols)
                for r in range(parts):
                    fresh = score(first[:, lanes], r, lanes)
                    mine[0, r] = fresh if q == 0 else mine[0, r] + fresh
                    if q == stages - 1:
                        if r == 0:
                            pl.semaphore_wait(barrier, greeted)
                        pair_copy(0, r).start()

    def second_scores():
        def step(m):
            group = along(m)
            with scope("midwait"):
                @pl.when(lead)
                def _():
                    awaited(middle.at[pl.ds(0, inner - 1)], mid_recv.at[group])
                    middle[group * inner + spot] = columns[group, head]

                @pl.when(follow)
                def _():
                    awaited(middle.at[pl.ds(0, inner)], mid_recv.at[group])

            left = jnp.concatenate([middle[group * inner + c] for c in range(inner)], axis=1)
            lanes = pl.ds(pl.multiple_of(group * span, 128), span)
            with scope("score"):
                for r in range(parts):
                    fresh = score(left, r, lanes)
                    if isinstance(m, int) and m == 0:
                        mine[1, r] = fresh
                    else:
                        mine[1, r] = mine[1, r] + fresh
                    if isinstance(m, int) and m == outer - 1:
                        pair_copy(1, r).start()

        step(0)
        loop(1, outer - 1, step)
        step(outer - 1)

    def share(group):
        for k in list(range(1, inner)) + [0]:
            for g in range(genes):
                if k > 0 or g != head:
                    mid_copy(group, g, k).start()

    def iteration(it):
        if it == 0:
            first_scores()
        else:
            second_scores()

        with scope("merge"):
            peak = None
            for r in range(parts):
                pair_copy(it, r).wait_recv()
                whole = mine[it, r] + theirs[it, r]
                most = jnp.max(jnp.abs(whole), axis=1, keepdims=True)
                peak = most if peak is None else jnp.maximum(peak, most)
                pieces = split_three(whole)
                for i in range(it + 2):
                    stacked[i * width : (i + 1) * width, part(r)] = pieces[i]

            peak = jnp.maximum(peak, 1e-30)
            lines_out[it] = turn(peak)
            shrink = jnp.broadcast_to(1.0 / peak, (width, chunk))
            for k in range(1, inner):
                line_copy(it, k).start()

            @pl.when(follow)
            def _():
                line_copy(it, 0).start()

        def gram():
            whole = stacked[0 : (it + 2) * width, :]
            cross = lax.dot_general(
                whole, whole, (((1,), (1,)), ((), ())), preferred_element_type=jnp.float32
            )
            cross = sum(cross[i * width : (i + 1) * width] for i in range(it + 2))
            total = sum(cross[:, i * width : (i + 1) * width] for i in range(it + 2))
            grams[it, spot] = jnp.concatenate([total[:half], total[half:]], axis=1)
            for k in range(inner):
                gram_copy(it, k).start()

        def product(lanes):
            wide = jnp.dot(
                stacked[0 : 2 * width, :], dense[:, lanes], preferred_element_type=jnp.float32
            )
            return wide[:width] + wide[width:]

        def dispatch(group, k, value):
            coded, steps = encode(value * shrink)
            codes_out[it, group, k] = coded
            steps_out[it, group, k] = steps

        def send(group, k):
            step_copy(it, group, k).start()
            near_copy(it, group, k).start()

        def multiply(m):
            group = along(outer - m)
            if isinstance(m, int) and m == 1 and chunk % side == 0:
                for k in list(range(1, inner)) + [0]:
                    at = (group * inner + lax.rem(spot + k, inner)) * chunk
                    value = product(pl.ds(pl.multiple_of(at, side), chunk))
                    sums_near[group, lax.rem(spot + k, inner)] = value
                    dispatch(group, k, value)
                    if k > 0:
                        send(group, k)
            else:
                wide = product(pl.ds(pl.multiple_of(group * span, 128), span))
                for c in range(inner):
                    sums_near[group, c] = wide[:, c * chunk : (c + 1) * chunk]
                for k in range(inner):
                    dispatch(group, k, sums_near[group, lax.rem(spot + k, inner)])
                for k in range(1, inner):
                    send(group, k)

            @pl.when(follow)
            def _():
                send(group, 0)

        def forward(m):
            group = along(outer - m)
            own = isinstance(m, int) and m == outer
            for g in range(genes):
                low = 1 if g == head else 0
                awaited(steps_in.at[it, g, group, pl.ds(low, inner - low)], step_recv.at[g, group])
                awaited(codes_in.at[it, g, group, pl.ds(low, inner - low)], near_recv.at[g, group])
                total = sums_near[group, spot] if g == head else None
                for k in range(low, inner):
                    value = decode(codes_in[it, g, group, k], steps_in[it, g, group, k]) * factors[g, k]
                    total = value if total is None else total + value
                if own:
                    sums_own[g] = total
                else:
                    coded, steps = encode(total * gains[g])
                    far_out[it, group, g] = coded
                    fars_out[it, group, g] = steps
            if not own:
                fars_copy(it, group).start()
                far_copy(it, group).start()

        def reduce():
            with scope("lines"):
                for g in range(genes):
                    low = 1 if g == head else 0
                    awaited(lines_in.at[it, g, pl.ds(low, inner - low)], line_recv.at[it, g])
                    tail = lines_out[it] if g == head else None
                    for k in range(low, inner):
                        line = lines_in[it, g, k]
                        tail = line if tail is None else tail + line
                        factors[g, k] = turn_back(line, chunk)
                    tails_out[it, g] = tail
                    gains[g] = turn_back(1.0 / tail, chunk)
                for k in range(1, outer):
                    tail_copy(it, k).start()
            with scope("gramwait"):
                awaited(grams.at[it], gram_recv.at[it])
            planes[it, here] = added(grams.at[it], inner)
            for k in range(1, outer):
                plane_copy(it, k).start()
            with scope("forward"):
                loop(1, outer, forward)
                forward(outer)
            with scope("planewait"):
                awaited(planes.at[it, pl.ds(0, outer - 1)], plane_recv.at[it])
            awaited(tails_in.at[it, pl.ds(0, outer - 1)], tail_recv.at[it])
            for g in range(genes):
                for k in range(1, outer):
                    stretch[g, k] = turn_back(tails_in[it, lax.rem(here + k, outer), g], chunk)
            total = added(planes.at[it], outer)
            total = jnp.concatenate([total[:, :width], total[:, width:]], axis=0)
            with scope("inverse"):
                inverse = inverse_factor(total)
            if it == 1:
                factor[...] = inverse
                remote(factor, factor, factor_send.at[0], factor_recv.at[0], gene=other).start()
            with scope("farwait"):
                awaited(fars_in.at[it, pl.ds(0, outer - 1)], fars_recv.at[it])
                awaited(far_in.at[it, pl.ds(0, outer - 1)], far_recv.at[it])
            with scope("result"):
                summed = []
                for g in range(genes):
                    part_sum = sums_own[g]
                    for k in range(1, outer):
                        source = lax.rem(here + k, outer)
                        value = decode(far_in[it, source, g], fars_in[it, source, g])
                        part_sum = part_sum + value * stretch[g, k]
                    summed.append(part_sum)
                summed = jnp.concatenate(summed, axis=1)
                result = jnp.dot(
                    inverse, summed, precision=HIGH, preferred_element_type=jnp.float32
                )
                result = [result[:, g * chunk : (g + 1) * chunk] for g in range(genes)]
                if it == 0:
                    for g in range(genes):
                        columns[here, g] = result[g].astype(columns.dtype)
                    for m in range(outer - 1, 0, -1):
                        column_copy(along(m)).start()
                    share(here)
                else:
                    load_res[...] = result[0]
                    remote(load_res, load_in, load_send.at[0], load_recv.at[0], gene=other).start()
                    load_out[...] = result[head]
            if it == 0:
                def relay(m):
                    group = along(m)
                    with scope("columnwait"):
                        awaited(columns.at[group], column_recv.at[group])
                    share(group)

                loop(1, outer, relay)

        with scope("gram"):
            pl.when(follow)(gram)
        with scope("multiply"):
            loop(1, outer + 1, multiply)
        pl.when(lead)(reduce)

    iteration(0)
    iteration(1)

    @pl.when(follow)
    def _():
        with scope("factorwait"):
            awaited(factor, factor_recv.at[0])

    with scope("finish"):
        scale = jnp.sqrt(jnp.float32(cells * cell_dev))
        left = jnp.concatenate(
            [jnp.concatenate([p] * 3, axis=1) for p in split_three(factor[...])], axis=0
        )
        for r in range(parts):
            final = jnp.dot(left, stacked[:, part(r)], preferred_element_type=jnp.float32)
            final = final[:width] + final[width : 2 * width] + final[2 * width :]
            basis_out[:, part(r)] = (final * scale).astype(basis_out.dtype)

    @pl.when(follow)
    def _():
        with scope("loadwait"):
            awaited(load_in, load_recv.at[0])
        load_out[...] = load_in[...]
        drained(codes_out, near_send.at[0])
        drained(steps_out, step_send.at[0])
        drained(grams, gram_send.at[0])
        drained(lines_in.at[:, 0], line_send.at[0])

    @pl.when(lead)
    def _():
        drained(codes_out.at[:, :, pl.ds(1, inner - 1)], near_send.at[0])
        drained(steps_out.at[:, :, pl.ds(1, inner - 1)], step_send.at[0])
        drained(lines_in.at[:, 0, pl.ds(1, inner - 1)], line_send.at[0])
        drained(planes.at[:, pl.ds(0, outer - 1)], plane_send.at[0])
        drained(far_in.at[:, pl.ds(0, outer - 1)], far_send.at[0])
        drained(fars_in.at[:, pl.ds(0, outer - 1)], fars_send.at[0])
        drained(tails_in.at[:, pl.ds(0, outer - 1)], tail_send.at[0])
        drained(columns.at[pl.ds(0, outer - 1)], column_send.at[0])
        loop(0, outer, lambda group: drained(
            middle.at[pl.ds(0, inner * genes - 1)], mid_send.at[group]
        ))
        drained(factor, factor_send.at[0])
        drained(load_res, load_send.at[0])

    drained(mine, pair_send.at[0])


def local(cells, genes, tiles, tile_row, tile_col, tile_count, start_basis):
    slots, side = tiles.shape[1], tiles.shape[-1]
    width, gene_dev = start_basis.shape
    gene_blocks = gene_dev // side
    cell_dev = ROW_BLOCKS * side
    chunk = gene_dev // cells
    parts = 2
    inner = 1
    while inner * inner * 4 <= cells and cells % (inner * 2) == 0:
        inner = inner * 2
    outer = cells // inner
    places = ROW_BLOCKS * gene_blocks
    dma = pltpu.SemaphoreType.DMA
    shapes = (
        jax.ShapeDtypeStruct((width, cell_dev), jnp.bfloat16),
        jax.ShapeDtypeStruct((width, chunk), jnp.float32),
    )
    results = pl.pallas_call(
        functools.partial(kernel, cells, inner, genes, parts),
        out_shape=shapes,
        in_specs=[
            pl.BlockSpec(memory_space=pltpu.SMEM),
            pl.BlockSpec(memory_space=pltpu.HBM),
            pl.BlockSpec(memory_space=pltpu.HBM),
            pl.BlockSpec(memory_space=pltpu.HBM),
            pl.BlockSpec(memory_space=pltpu.HBM),
        ],
        out_specs=(
            pl.BlockSpec(memory_space=pltpu.VMEM),
            pl.BlockSpec(memory_space=pltpu.VMEM),
        ),
        scratch_shapes=[
            pltpu.VMEM((2, 1, slots), jnp.int32),
            pltpu.VMEM((1, places), jnp.int32),
            pltpu.SMEM((1, places), jnp.int32),
            pltpu.VMEM((slots + 1, side, side), jnp.bfloat16),
            pltpu.VMEM((cell_dev, gene_dev), jnp.bfloat16),
            pltpu.VMEM((width, gene_dev), jnp.bfloat16),
            pltpu.VMEM((2, parts, width, cell_dev // parts), jnp.float32),
            pltpu.VMEM((2, parts, width, cell_dev // parts), jnp.float32),
            pltpu.VMEM((3 * width, cell_dev), jnp.bfloat16),
            pltpu.VMEM((2, inner, width // 2, 2 * width), jnp.float32),
            pltpu.VMEM((2, outer, width // 2, 2 * width), jnp.float32),
            pltpu.VMEM((width, width), jnp.float32),
            pltpu.VMEM((outer, inner, width, chunk), jnp.float32),
            pltpu.VMEM((2, outer, inner, width, chunk), jnp.int16),
            pltpu.VMEM((2, genes, outer, inner, width, chunk), jnp.int16),
            pltpu.VMEM((2, outer, inner, 1, chunk), jnp.float32),
            pltpu.VMEM((2, genes, outer, inner, 1, chunk), jnp.float32),
            pltpu.VMEM((2, 1, width), jnp.float32),
            pltpu.VMEM((2, genes, inner, 1, width), jnp.float32),
            pltpu.VMEM((genes, inner, width, chunk), jnp.float32),
            pltpu.VMEM((genes, width, chunk), jnp.float32),
            pltpu.VMEM((2, outer, genes, width, chunk), jnp.int16),
            pltpu.VMEM((2, outer, genes, width, chunk), jnp.int16),
            pltpu.VMEM((2, outer, genes, 1, chunk), jnp.float32),
            pltpu.VMEM((2, outer, genes, 1, chunk), jnp.float32),
            pltpu.VMEM((2, genes, 1, width), jnp.float32),
            pltpu.VMEM((2, outer, genes, 1, width), jnp.float32),
            pltpu.VMEM((genes, width, chunk), jnp.float32),
            pltpu.VMEM((genes, outer, width, chunk), jnp.float32),
            pltpu.VMEM((outer, genes, width, chunk), jnp.bfloat16),
            pltpu.VMEM((cells, width, chunk), jnp.bfloat16),
            pltpu.VMEM((width, chunk), jnp.float32),
            pltpu.VMEM((width, chunk), jnp.float32),
            dma, dma((2,)), dma, dma,
            dma((1,)), dma((2, parts)),
            dma((1,)), dma((2,)), dma((1,)), dma((2,)), dma((1,)), dma((1,)),
            dma((1,)), dma((genes, outer)), dma((1,)), dma((genes, outer)),
            dma((1,)), dma((2, genes)),
            dma((1,)), dma((2,)), dma((1,)), dma((2,)), dma((1,)), dma((2,)),
            dma((1,)), dma((outer,)), dma((outer,)), dma((outer,)), dma((1,)), dma((1,)),
        ],
        compiler_params=pltpu.CompilerParams(
            collective_id=0, has_side_effects=True, vmem_limit_bytes=44 * 1024 * 1024
        ),
    )(tile_count, *(
        pltpu.with_memory_space_constraint(array, pltpu.HBM)
        for array in (tile_row, tile_col, tiles[0], start_basis)
    ))
    return pl.pallas_call(
        deliver,
        out_shape=shapes,
        in_specs=[pl.BlockSpec(memory_space=pltpu.VMEM)] * 2,
        out_specs=(pl.BlockSpec(memory_space=pl.ANY),) * 2,
        scratch_shapes=[dma((2,))],
        compiler_params=pltpu.CompilerParams(vmem_limit_bytes=1024 * 1024),
    )(*results)


def deliver(basis, load, basis_out, load_out, sems):
    copies = [
        pltpu.make_async_copy(basis, basis_out, sems.at[0]),
        pltpu.make_async_copy(load, load_out, sems.at[1]),
    ]
    for copy in copies:
        copy.start()
    for copy in copies:
        copy.wait()


def solution(mesh):
    return jax.shard_map(
        functools.partial(local, mesh.shape["cell"], mesh.shape["gene"]),
        mesh=mesh,
        in_specs=(
            P("gene", "cell", None, None),
            P("gene", "cell"),
            P("gene", "cell"),
            P("gene", "cell"),
            P(None, "gene"),
        ),
        out_specs=(P(None, "cell"), P(None, ("gene", "cell"))),
        check_vma=False,
    )
```

```python
import functools

import jax
import jax.numpy as jnp
from jax import lax
from jax.experimental import pallas as pl
from jax.experimental.pallas import tpu as pltpu
from jax.sharding import PartitionSpec as P

ROW_BLOCKS = 8
PANEL = 8
LEVELS = 32766.0
MESH = pl.DeviceIdType.MESH
HIGH = lax.Precision.HIGHEST
scope = jax.named_scope


def split_three(value):
    high = value.astype(jnp.bfloat16)
    rest = value - high.astype(jnp.float32)
    middle = rest.astype(jnp.bfloat16)
    low = (rest - middle.astype(jnp.float32)).astype(jnp.bfloat16)
    return high, middle, low


def inverse_factor(gram):
    width = gram.shape[0]
    shape = (width, 2 * width)
    row = lax.broadcasted_iota(jnp.int32, shape, 0)
    lane = lax.broadcasted_iota(jnp.int32, shape, 1)
    both = jnp.concatenate([jnp.zeros_like(gram), gram], axis=1)
    both = jnp.where(row == lane, 1.0, both)
    pivots = jnp.ones(shape, jnp.float32)
    done = []
    start = 0

    def spread(first):
        return {
            j: jnp.broadcast_to(both[:, width + j : width + j + 1], both.shape)
            for j in range(first, min(first + PANEL, width))
        }

    ahead = spread(0)
    for first in range(0, width, PANEL):
        base = first // 8 * 8
        if base > start:
            done.append((both[: base - start], pivots[: base - start]))
            both = both[base - start :]
            pivots = pivots[base - start :]
            row = row[base - start :]
            ahead = {j: column[base - start :] for j, column in ahead.items()}
            start = base
        columns = ahead
        ahead = spread(first + PANEL)
        for j in range(first, first + PANEL):
            at = j - start
            column = columns.pop(j)
            pivot = column[at : at + 1]
            factor = jnp.where(row > j, column * (1.0 / pivot), 0.0)
            pivots = jnp.where(row == j, pivot, pivots)
            both = both - factor * both[at : at + 1]
            for later in (columns, ahead):
                for m in later:
                    later[m] = later[m] - factor * later[m][at : at + 1]
    done.append((both, pivots))
    both = jnp.concatenate([piece for piece, _ in done], axis=0)
    pivots = jnp.concatenate([piece for _, piece in done], axis=0)
    return (both * lax.rsqrt(pivots))[:, :width]


def diagonal(width):
    square = (width, width)
    return lax.broadcasted_iota(jnp.int32, square, 0) == lax.broadcasted_iota(jnp.int32, square, 1)


def turn(column):
    square = (column.shape[0], column.shape[0])
    turned = jnp.where(diagonal(square[0]), jnp.broadcast_to(column, square), 0.0)
    return jnp.sum(turned, axis=0, keepdims=True)


def turn_back(line, lanes):
    square = (line.shape[1], line.shape[1])
    turned = jnp.where(diagonal(square[0]), jnp.broadcast_to(line, square), 0.0)
    return jnp.broadcast_to(jnp.sum(turned, axis=1, keepdims=True), (square[0], lanes))


def encode(value):
    peak = jnp.max(jnp.abs(value), axis=0, keepdims=True)
    step = jnp.maximum(peak, 1e-30) * (1.0 / LEVELS)
    return jnp.round(value * (1.0 / step)).astype(jnp.int32).astype(jnp.int16), step


def decode(coded, step):
    return coded.astype(jnp.int32).astype(jnp.float32) * step


def kernel(
    cells, inner, genes, parts,
    slot_count, slot_row, slot_col, tiles, start, basis_out, load_out,
    slots_in, places_out, table, held, dense, first, mine, theirs, stacked, grams, planes, factor,
    sums_near, codes_out, codes_in, steps_out, steps_in, lines_out, lines_in, factors,
    sums_own, far_out, far_in, fars_out, fars_in, tails_out, tails_in, gains, stretch,
    columns, middle, load_res, load_in,
    tile_sem, slot_sem, table_sem, start_sem, pair_send, pair_recv,
    gram_send, gram_recv, plane_send, plane_recv, factor_send, factor_recv,
    near_send, near_recv, step_send, step_recv, line_send, line_recv,
    far_send, far_recv, fars_send, fars_recv, tail_send, tail_recv,
    column_send, column_recv, mid_send, mid_recv, load_send, load_recv,
):
    cell = lax.axis_index("cell")
    gene = lax.axis_index("gene")
    slots, side, _ = tiles.shape
    width = start.shape[0]
    cell_dev, gene_dev = dense.shape
    gene_blocks = gene_dev // side
    chunk = gene_dev // cells
    piece = cell_dev // parts
    half = width // 2
    outer = cells // inner
    span = inner * chunk
    here = cell // inner
    spot = lax.rem(cell, inner)
    other = lax.rem(gene + 1, genes)
    head = genes - 1
    lead = gene == head
    follow = gene != head

    slot_copies = [
        pltpu.make_async_copy(slot_row, slots_in.at[0], slot_sem.at[0]),
        pltpu.make_async_copy(slot_col, slots_in.at[1], slot_sem.at[1]),
    ]
    for copy in slot_copies:
        copy.start()
    fetch = pltpu.make_async_copy(tiles, held.at[pl.ds(0, slots)], tile_sem)
    fetch.start()
    first_basis = pltpu.make_async_copy(start, first, start_sem)
    first_basis.start()

    def near(k):
        return here * inner + lax.rem(spot + k, inner)

    def far(k):
        return lax.rem(here + k, outer) * inner + spot

    barrier = pltpu.get_barrier_semaphore()
    greeted = 0
    for k in range(inner):
        for g in range(genes):
            if k + g > 0:
                pl.semaphore_signal(
                    barrier, inc=1,
                    device_id={"cell": near(k), "gene": lax.rem(gene + g, genes)},
                    device_id_type=MESH,
                )
                greeted += 1
    for k in range(1, outer):
        pl.semaphore_signal(barrier, inc=1, device_id={"cell": far(k)}, device_id_type=MESH)
        greeted += 1

    held[slots] = jnp.zeros((side, side), held.dtype)
    for copy in slot_copies:
        copy.wait()
    places = (cell_dev // side) * gene_blocks
    lane = lax.broadcasted_iota(jnp.int32, (1, slots), 1)
    spots = jnp.where(
        lane < slot_count[0, 0], slots_in[0] * gene_blocks + slots_in[1], places
    )
    square = (slots, slots)
    turned = jnp.where(diagonal(slots), jnp.broadcast_to(spots, square), 0)
    turned = jnp.sum(turned, axis=1, keepdims=True)
    flat = (slots, places)
    found = jnp.broadcast_to(turned, flat) == lax.broadcasted_iota(jnp.int32, flat, 1)
    found = jnp.where(found, lax.broadcasted_iota(jnp.int32, flat, 0), slots)
    places_out[...] = jnp.min(found, axis=0, keepdims=True)
    listing = pltpu.make_async_copy(places_out, table, table_sem)
    listing.start()
    listing.wait()
    fetch.wait()
    first_basis.wait()

    def remote(source, target, send_sem, recv_sem, **device):
        return pltpu.make_async_remote_copy(
            src_ref=source, dst_ref=target, send_sem=send_sem, recv_sem=recv_sem,
            device_id=device, device_id_type=MESH,
        )

    def pair_copy(it, r):
        return remote(
            mine.at[it, r], theirs.at[it, r], pair_send.at[0], pair_recv.at[it, r], gene=other
        )

    def gram_copy(it, k):
        return remote(
            grams.at[it, spot], grams.at[it, spot], gram_send.at[0], gram_recv.at[it],
            cell=near(k), gene=head,
        )

    def plane_copy(it, k):
        return remote(
            planes.at[it, here], planes.at[it, here], plane_send.at[0], plane_recv.at[it],
            cell=far(k),
        )

    def near_copy(it, group, k):
        return remote(
            codes_out.at[it, group, k], codes_in.at[it, gene, group, k],
            near_send.at[0], near_recv.at[gene, group], cell=near(k), gene=head,
        )

    def step_copy(it, group, k):
        return remote(
            steps_out.at[it, group, k], steps_in.at[it, gene, group, k],
            step_send.at[0], step_recv.at[gene, group], cell=near(k), gene=head,
        )

    def line_copy(it, k):
        return remote(
            lines_out.at[it], lines_in.at[it, gene, k],
            line_send.at[0], line_recv.at[it, gene], cell=near(k), gene=head,
        )

    def far_copy(it, group):
        return remote(
            far_out.at[it, group], far_in.at[it, here],
            far_send.at[0], far_recv.at[it], cell=group * inner + spot,
        )

    def fars_copy(it, group):
        return remote(
            fars_out.at[it, group], fars_in.at[it, here],
            fars_send.at[0], fars_recv.at[it], cell=group * inner + spot,
        )

    def tail_copy(it, k):
        return remote(
            tails_out.at[it], tails_in.at[it, here],
            tail_send.at[0], tail_recv.at[it], cell=far(k),
        )

    def column_copy(target):
        return remote(
            columns.at[here], columns.at[here], column_send.at[0], column_recv.at[here],
            cell=target * inner + spot,
        )

    def mid_copy(group, g, k):
        return remote(
            columns.at[group, g], middle.at[group * inner + spot],
            mid_send.at[group], mid_recv.at[group], cell=near(k), gene=g,
        )

    def awaited(refs, sem):
        remote(refs, refs, pair_send.at[0], sem, gene=other).wait_recv()

    def drained(refs, sem):
        remote(refs, refs, sem, pair_recv.at[0, 0], gene=other).wait_send()

    def added(ref, count):
        total = ref[0]
        for c in range(1, count):
            total = total + ref[c]
        return total

    def loop(first, last, act):
        if last - first <= 4:
            for k in range(first, last):
                act(k)
        else:
            def body(k, _):
                act(k)
                return 0

            lax.fori_loop(first, last, body, 0)

    def part(r):
        return pl.ds(r * piece, piece)

    def along(m):
        return lax.rem(here + jnp.where(2 * here < outer, m, outer - m), outer)

    def place(low, high):
        for row in range(cell_dev // side):
            for col in range(low, high):
                dense[row * side : (row + 1) * side, col * side : (col + 1) * side] = held[
                    table[0, row * gene_blocks + col]
                ]

    def score(left, r, lanes):
        return lax.dot_general(
            left, dense[part(r), lanes], (((1,), (1,)), ((), ())),
            preferred_element_type=jnp.float32,
        )

    def first_scores():
        stages = 4
        share_cols = gene_blocks // stages
        with scope("place"):
            place(0, share_cols)
        for q in range(stages):
            lanes = slice(q * share_cols * side, (q + 1) * share_cols * side)
            with scope("score"):
                if q + 1 < stages:
                    place((q + 1) * share_cols, (q + 2) * share_cols)
                for r in range(parts):
                    fresh = score(first[:, lanes], r, lanes)
                    mine[0, r] = fresh if q == 0 else mine[0, r] + fresh
                    if q == stages - 1:
                        if r == 0:
                            pl.semaphore_wait(barrier, greeted)
                        pair_copy(0, r).start()

    def second_scores():
        def step(m):
            group = along(m)
            with scope("midwait"):
                @pl.when(lead)
                def _():
                    awaited(middle.at[pl.ds(0, inner - 1)], mid_recv.at[group])
                    middle[group * inner + spot] = columns[group, head]

                @pl.when(follow)
                def _():
                    awaited(middle.at[pl.ds(0, inner)], mid_recv.at[group])

            left = jnp.concatenate([middle[group * inner + c] for c in range(inner)], axis=1)
            lanes = pl.ds(pl.multiple_of(group * span, 128), span)
            with scope("score"):
                for r in range(parts):
                    fresh = score(left, r, lanes)
                    if isinstance(m, int) and m == 0:
                        mine[1, r] = fresh
                    else:
                        mine[1, r] = mine[1, r] + fresh
                    if isinstance(m, int) and m == outer - 1:
                        pair_copy(1, r).start()

        step(0)
        loop(1, outer - 1, step)
        step(outer - 1)

    def share(group):
        for k in list(range(1, inner)) + [0]:
            for g in range(genes):
                if k > 0 or g != head:
                    mid_copy(group, g, k).start()

    def iteration(it):
        if it == 0:
            first_scores()
        else:
            second_scores()

        with scope("merge"):
            peak = None
            for r in range(parts):
                pair_copy(it, r).wait_recv()
                whole = mine[it, r] + theirs[it, r]
                most = jnp.max(jnp.abs(whole), axis=1, keepdims=True)
                peak = most if peak is None else jnp.maximum(peak, most)
                pieces = split_three(whole)
                for i in range(it + 2):
                    stacked[i * width : (i + 1) * width, part(r)] = pieces[i]

            peak = jnp.maximum(peak, 1e-30)
            lines_out[it] = turn(peak)
            shrink = jnp.broadcast_to(1.0 / peak, (width, chunk))
            for k in range(1, inner):
                line_copy(it, k).start()

            @pl.when(follow)
            def _():
                line_copy(it, 0).start()

        def gram():
            whole = stacked[0 : (it + 2) * width, :]
            cross = lax.dot_general(
                whole, whole, (((1,), (1,)), ((), ())), preferred_element_type=jnp.float32
            )
            cross = sum(cross[i * width : (i + 1) * width] for i in range(it + 2))
            total = sum(cross[:, i * width : (i + 1) * width] for i in range(it + 2))
            grams[it, spot] = jnp.concatenate([total[:half], total[half:]], axis=1)
            for k in range(inner):
                gram_copy(it, k).start()

        def product(lanes):
            wide = jnp.dot(
                stacked[0 : 2 * width, :], dense[:, lanes], preferred_element_type=jnp.float32
            )
            return wide[:width] + wide[width:]

        def dispatch(group, k, value):
            coded, steps = encode(value * shrink)
            codes_out[it, group, k] = coded
            steps_out[it, group, k] = steps

        def send(group, k):
            step_copy(it, group, k).start()
            near_copy(it, group, k).start()

        def multiply(m):
            group = along(outer - m)

            def by_chunk():
                for k in list(range(1, inner)) + [0]:
                    at = (group * inner + lax.rem(spot + k, inner)) * chunk
                    value = product(pl.ds(pl.multiple_of(at, side), chunk))
                    dispatch(group, k, value)
                    send(group, k)

            def whole_group():
                wide = product(pl.ds(pl.multiple_of(group * span, 128), span))
                for c in range(inner):
                    sums_near[group, c] = wide[:, c * chunk : (c + 1) * chunk]
                for k in range(inner):
                    dispatch(group, k, sums_near[group, lax.rem(spot + k, inner)])
                for k in range(1, inner):
                    send(group, k)

            if isinstance(m, int) and m == 1 and chunk % side == 0:
                pl.when(follow)(by_chunk)

                @pl.when(lead)
                def _():
                    whole_group()

                return
            whole_group()

            @pl.when(follow)
            def _():
                send(group, 0)

        def forward(m):
            group = along(outer - m)
            own = isinstance(m, int) and m == outer
            for g in range(genes):
                low = 1 if g == head else 0
                awaited(steps_in.at[it, g, group, pl.ds(low, inner - low)], step_recv.at[g, group])
                awaited(codes_in.at[it, g, group, pl.ds(low, inner - low)], near_recv.at[g, group])
                total = sums_near[group, spot] if g == head else None
                for k in range(low, inner):
                    value = decode(codes_in[it, g, group, k], steps_in[it, g, group, k]) * factors[g, k]
                    total = value if total is None else total + value
                if own:
                    sums_own[g] = total
                else:
                    coded, steps = encode(total * gains[g])
                    far_out[it, group, g] = coded
                    fars_out[it, group, g] = steps
            if not own:
                fars_copy(it, group).start()
                far_copy(it, group).start()

        def reduce():
            with scope("lines"):
                for g in range(genes):
                    low = 1 if g == head else 0
                    awaited(lines_in.at[it, g, pl.ds(low, inner - low)], line_recv.at[it, g])
                    tail = lines_out[it] if g == head else None
                    for k in range(low, inner):
                        line = lines_in[it, g, k]
                        tail = line if tail is None else tail + line
                        factors[g, k] = turn_back(line, chunk)
                    tails_out[it, g] = tail
                    gains[g] = turn_back(1.0 / tail, chunk)
                for k in range(1, outer):
                    tail_copy(it, k).start()
            with scope("gramwait"):
                awaited(grams.at[it], gram_recv.at[it])
            planes[it, here] = added(grams.at[it], inner)
            for k in range(1, outer):
                plane_copy(it, k).start()
            with scope("forward"):
                loop(1, outer, forward)
                forward(outer)
            with scope("planewait"):
                awaited(planes.at[it, pl.ds(0, outer - 1)], plane_recv.at[it])
            awaited(tails_in.at[it, pl.ds(0, outer - 1)], tail_recv.at[it])
            for g in range(genes):
                for k in range(1, outer):
                    stretch[g, k] = turn_back(tails_in[it, lax.rem(here + k, outer), g], chunk)
            total = added(planes.at[it], outer)
            total = jnp.concatenate([total[:, :width], total[:, width:]], axis=0)
            with scope("inverse"):
                inverse = inverse_factor(total)
            if it == 1:
                factor[...] = inverse
                remote(factor, factor, factor_send.at[0], factor_recv.at[0], gene=other).start()
            with scope("farwait"):
                awaited(fars_in.at[it, pl.ds(0, outer - 1)], fars_recv.at[it])
                awaited(far_in.at[it, pl.ds(0, outer - 1)], far_recv.at[it])
            with scope("result"):
                summed = []
                for g in range(genes):
                    part_sum = sums_own[g]
                    for k in range(1, outer):
                        source = lax.rem(here + k, outer)
                        value = decode(far_in[it, source, g], fars_in[it, source, g])
                        part_sum = part_sum + value * stretch[g, k]
                    summed.append(part_sum)
                summed = jnp.concatenate(summed, axis=1)
                result = jnp.dot(
                    inverse, summed, precision=HIGH, preferred_element_type=jnp.float32
                )
                result = [result[:, g * chunk : (g + 1) * chunk] for g in range(genes)]
                if it == 0:
                    for g in range(genes):
                        columns[here, g] = result[g].astype(columns.dtype)
                    for m in range(outer - 1, 0, -1):
                        column_copy(along(m)).start()
                    share(here)
                else:
                    load_res[...] = result[0]
                    remote(load_res, load_in, load_send.at[0], load_recv.at[0], gene=other).start()
                    load_out[...] = result[head]
            if it == 0:
                def relay(m):
                    group = along(m)
                    with scope("columnwait"):
                        awaited(columns.at[group], column_recv.at[group])
                    share(group)

                loop(1, outer, relay)

        with scope("gram"):
            pl.when(follow)(gram)
        with scope("multiply"):
            loop(1, outer + 1, multiply)
        pl.when(lead)(reduce)

    iteration(0)
    iteration(1)

    @pl.when(follow)
    def _():
        with scope("factorwait"):
            awaited(factor, factor_recv.at[0])

    with scope("finish"):
        scale = jnp.sqrt(jnp.float32(cells * cell_dev))
        left = jnp.concatenate(
            [jnp.concatenate([p] * 3, axis=1) for p in split_three(factor[...])], axis=0
        )
        for r in range(parts):
            final = jnp.dot(left, stacked[:, part(r)], preferred_element_type=jnp.float32)
            final = final[:width] + final[width : 2 * width] + final[2 * width :]
            basis_out[:, part(r)] = (final * scale).astype(basis_out.dtype)

    @pl.when(follow)
    def _():
        with scope("loadwait"):
            awaited(load_in, load_recv.at[0])
        load_out[...] = load_in[...]
        drained(codes_out, near_send.at[0])
        drained(steps_out, step_send.at[0])
        drained(grams, gram_send.at[0])
        drained(lines_in.at[:, 0], line_send.at[0])

    @pl.when(lead)
    def _():
        drained(codes_out.at[:, :, pl.ds(1, inner - 1)], near_send.at[0])
        drained(steps_out.at[:, :, pl.ds(1, inner - 1)], step_send.at[0])
        drained(lines_in.at[:, 0, pl.ds(1, inner - 1)], line_send.at[0])
        drained(planes.at[:, pl.ds(0, outer - 1)], plane_send.at[0])
        drained(far_in.at[:, pl.ds(0, outer - 1)], far_send.at[0])
        drained(fars_in.at[:, pl.ds(0, outer - 1)], fars_send.at[0])
        drained(tails_in.at[:, pl.ds(0, outer - 1)], tail_send.at[0])
        drained(columns.at[pl.ds(0, outer - 1)], column_send.at[0])
        loop(0, outer, lambda group: drained(
            middle.at[pl.ds(0, inner * genes - 1)], mid_send.at[group]
        ))
        drained(factor, factor_send.at[0])
        drained(load_res, load_send.at[0])

    drained(mine, pair_send.at[0])


def local(cells, genes, tiles, tile_row, tile_col, tile_count, start_basis):
    slots, side = tiles.shape[1], tiles.shape[-1]
    width, gene_dev = start_basis.shape
    gene_blocks = gene_dev // side
    cell_dev = ROW_BLOCKS * side
    chunk = gene_dev // cells
    parts = 2
    inner = 1
    while inner * inner * 4 <= cells and cells % (inner * 2) == 0:
        inner = inner * 2
    outer = cells // inner
    places = ROW_BLOCKS * gene_blocks
    dma = pltpu.SemaphoreType.DMA
    shapes = (
        jax.ShapeDtypeStruct((width, cell_dev), jnp.bfloat16),
        jax.ShapeDtypeStruct((width, chunk), jnp.float32),
    )
    results = pl.pallas_call(
        functools.partial(kernel, cells, inner, genes, parts),
        out_shape=shapes,
        in_specs=[
            pl.BlockSpec(memory_space=pltpu.SMEM),
            pl.BlockSpec(memory_space=pltpu.HBM),
            pl.BlockSpec(memory_space=pltpu.HBM),
            pl.BlockSpec(memory_space=pltpu.HBM),
            pl.BlockSpec(memory_space=pltpu.HBM),
        ],
        out_specs=(
            pl.BlockSpec(memory_space=pltpu.VMEM),
            pl.BlockSpec(memory_space=pltpu.VMEM),
        ),
        scratch_shapes=[
            pltpu.VMEM((2, 1, slots), jnp.int32),
            pltpu.VMEM((1, places), jnp.int32),
            pltpu.SMEM((1, places), jnp.int32),
            pltpu.VMEM((slots + 1, side, side), jnp.bfloat16),
            pltpu.VMEM((cell_dev, gene_dev), jnp.bfloat16),
            pltpu.VMEM((width, gene_dev), jnp.bfloat16),
            pltpu.VMEM((2, parts, width, cell_dev // parts), jnp.float32),
            pltpu.VMEM((2, parts, width, cell_dev // parts), jnp.float32),
            pltpu.VMEM((3 * width, cell_dev), jnp.bfloat16),
            pltpu.VMEM((2, inner, width // 2, 2 * width), jnp.float32),
            pltpu.VMEM((2, outer, width // 2, 2 * width), jnp.float32),
            pltpu.VMEM((width, width), jnp.float32),
            pltpu.VMEM((outer, inner, width, chunk), jnp.float32),
            pltpu.VMEM((2, outer, inner, width, chunk), jnp.int16),
            pltpu.VMEM((2, genes, outer, inner, width, chunk), jnp.int16),
            pltpu.VMEM((2, outer, inner, 1, chunk), jnp.float32),
            pltpu.VMEM((2, genes, outer, inner, 1, chunk), jnp.float32),
            pltpu.VMEM((2, 1, width), jnp.float32),
            pltpu.VMEM((2, genes, inner, 1, width), jnp.float32),
            pltpu.VMEM((genes, inner, width, chunk), jnp.float32),
            pltpu.VMEM((genes, width, chunk), jnp.float32),
            pltpu.VMEM((2, outer, genes, width, chunk), jnp.int16),
            pltpu.VMEM((2, outer, genes, width, chunk), jnp.int16),
            pltpu.VMEM((2, outer, genes, 1, chunk), jnp.float32),
            pltpu.VMEM((2, outer, genes, 1, chunk), jnp.float32),
            pltpu.VMEM((2, genes, 1, width), jnp.float32),
            pltpu.VMEM((2, outer, genes, 1, width), jnp.float32),
            pltpu.VMEM((genes, width, chunk), jnp.float32),
            pltpu.VMEM((genes, outer, width, chunk), jnp.float32),
            pltpu.VMEM((outer, genes, width, chunk), jnp.bfloat16),
            pltpu.VMEM((cells, width, chunk), jnp.bfloat16),
            pltpu.VMEM((width, chunk), jnp.float32),
            pltpu.VMEM((width, chunk), jnp.float32),
            dma, dma((2,)), dma, dma,
            dma((1,)), dma((2, parts)),
            dma((1,)), dma((2,)), dma((1,)), dma((2,)), dma((1,)), dma((1,)),
            dma((1,)), dma((genes, outer)), dma((1,)), dma((genes, outer)),
            dma((1,)), dma((2, genes)),
            dma((1,)), dma((2,)), dma((1,)), dma((2,)), dma((1,)), dma((2,)),
            dma((1,)), dma((outer,)), dma((outer,)), dma((outer,)), dma((1,)), dma((1,)),
        ],
        compiler_params=pltpu.CompilerParams(
            collective_id=0, has_side_effects=True, vmem_limit_bytes=44 * 1024 * 1024
        ),
    )(tile_count, *(
        pltpu.with_memory_space_constraint(array, pltpu.HBM)
        for array in (tile_row, tile_col, tiles[0], start_basis)
    ))
    return pl.pallas_call(
        deliver,
        out_shape=shapes,
        in_specs=[pl.BlockSpec(memory_space=pltpu.VMEM)] * 2,
        out_specs=(pl.BlockSpec(memory_space=pl.ANY),) * 2,
        scratch_shapes=[dma((2,))],
        compiler_params=pltpu.CompilerParams(vmem_limit_bytes=1024 * 1024),
    )(*results)


def deliver(basis, load, basis_out, load_out, sems):
    copies = [
        pltpu.make_async_copy(basis, basis_out, sems.at[0]),
        pltpu.make_async_copy(load, load_out, sems.at[1]),
    ]
    for copy in copies:
        copy.start()
    for copy in copies:
        copy.wait()


def solution(mesh):
    return jax.shard_map(
        functools.partial(local, mesh.shape["cell"], mesh.shape["gene"]),
        mesh=mesh,
        in_specs=(
            P("gene", "cell", None, None),
            P("gene", "cell"),
            P("gene", "cell"),
            P("gene", "cell"),
            P(None, "gene"),
        ),
        out_specs=(P(None, "cell"), P(None, ("gene", "cell"))),
        check_vma=False,
    )
```

```python
import functools

import jax
import jax.numpy as jnp
from jax import lax
from jax.experimental import pallas as pl
from jax.experimental.pallas import tpu as pltpu
from jax.sharding import PartitionSpec as P

ROW_BLOCKS = 8
PANEL = 8
LEVELS = 32766.0
MESH = pl.DeviceIdType.MESH
HIGH = lax.Precision.HIGHEST
scope = jax.named_scope


def split_three(value):
    high = value.astype(jnp.bfloat16)
    rest = value - high.astype(jnp.float32)
    middle = rest.astype(jnp.bfloat16)
    low = (rest - middle.astype(jnp.float32)).astype(jnp.bfloat16)
    return high, middle, low


def inverse_factor(gram):
    width = gram.shape[0]
    shape = (width, 2 * width)
    row = lax.broadcasted_iota(jnp.int32, shape, 0)
    lane = lax.broadcasted_iota(jnp.int32, shape, 1)
    both = jnp.concatenate([jnp.zeros_like(gram), gram], axis=1)
    both = jnp.where(row == lane, 1.0, both)
    pivots = jnp.ones(shape, jnp.float32)
    done = []
    start = 0

    def spread(first):
        return {
            j: jnp.broadcast_to(both[:, width + j : width + j + 1], both.shape)
            for j in range(first, min(first + PANEL, width))
        }

    ahead = spread(0)
    for first in range(0, width, PANEL):
        base = first // 8 * 8
        if base > start:
            done.append((both[: base - start], pivots[: base - start]))
            both = both[base - start :]
            pivots = pivots[base - start :]
            row = row[base - start :]
            ahead = {j: column[base - start :] for j, column in ahead.items()}
            start = base
        columns = ahead
        ahead = spread(first + PANEL)
        for j in range(first, first + PANEL):
            at = j - start
            column = columns.pop(j)
            pivot = column[at : at + 1]
            factor = jnp.where(row > j, column * (1.0 / pivot), 0.0)
            pivots = jnp.where(row == j, pivot, pivots)
            both = both - factor * both[at : at + 1]
            for later in (columns, ahead):
                for m in later:
                    later[m] = later[m] - factor * later[m][at : at + 1]
    done.append((both, pivots))
    both = jnp.concatenate([piece for piece, _ in done], axis=0)
    pivots = jnp.concatenate([piece for _, piece in done], axis=0)
    return (both * lax.rsqrt(pivots))[:, :width]


def diagonal(width):
    square = (width, width)
    return lax.broadcasted_iota(jnp.int32, square, 0) == lax.broadcasted_iota(jnp.int32, square, 1)


def turn(column):
    square = (column.shape[0], column.shape[0])
    turned = jnp.where(diagonal(square[0]), jnp.broadcast_to(column, square), 0.0)
    return jnp.sum(turned, axis=0, keepdims=True)


def turn_back(line, lanes):
    square = (line.shape[1], line.shape[1])
    turned = jnp.where(diagonal(square[0]), jnp.broadcast_to(line, square), 0.0)
    return jnp.broadcast_to(jnp.sum(turned, axis=1, keepdims=True), (square[0], lanes))


def encode(value):
    peak = jnp.max(jnp.abs(value), axis=0, keepdims=True)
    step = jnp.maximum(peak, 1e-30) * (1.0 / LEVELS)
    return jnp.round(value * (1.0 / step)).astype(jnp.int32).astype(jnp.int16), step


def decode(coded, step):
    return coded.astype(jnp.int32).astype(jnp.float32) * step


def kernel(
    cells, inner, genes, parts,
    slot_count, slot_row, slot_col, tiles, start, basis_out, load_out,
    slots_in, places_out, table, held, dense, first, mine, theirs, stacked, grams, planes, factor,
    sums_near, codes_out, codes_in, steps_out, steps_in, lines_out, lines_in, factors,
    sums_own, far_out, far_in, fars_out, fars_in, tails_out, tails_in, gains, stretch,
    columns, middle, load_res, load_in,
    tile_sem, slot_sem, table_sem, start_sem, pair_send, pair_recv,
    gram_send, gram_recv, plane_send, plane_recv, factor_send, factor_recv,
    near_send, near_recv, step_send, step_recv, line_send, line_recv,
    far_send, far_recv, fars_send, fars_recv, tail_send, tail_recv,
    column_send, column_recv, mid_send, mid_recv, load_send, load_recv,
):
    cell = lax.axis_index("cell")
    gene = lax.axis_index("gene")
    slots, side, _ = tiles.shape
    width = start.shape[0]
    cell_dev, gene_dev = dense.shape
    gene_blocks = gene_dev // side
    chunk = gene_dev // cells
    piece = cell_dev // parts
    half = width // 2
    outer = cells // inner
    span = inner * chunk
    here = cell // inner
    spot = lax.rem(cell, inner)
    other = lax.rem(gene + 1, genes)
    head = genes - 1
    lead = gene == head
    follow = gene != head

    slot_copies = [
        pltpu.make_async_copy(slot_row, slots_in.at[0], slot_sem.at[0]),
        pltpu.make_async_copy(slot_col, slots_in.at[1], slot_sem.at[1]),
    ]
    for copy in slot_copies:
        copy.start()
    fetch = pltpu.make_async_copy(tiles, held.at[pl.ds(0, slots)], tile_sem)
    fetch.start()
    first_basis = pltpu.make_async_copy(start, first, start_sem)
    first_basis.start()

    def near(k):
        return here * inner + lax.rem(spot + k, inner)

    def far(k):
        return lax.rem(here + k, outer) * inner + spot

    barrier = pltpu.get_barrier_semaphore()
    greeted = 0
    for k in range(inner):
        for g in range(genes):
            if k + g > 0:
                pl.semaphore_signal(
                    barrier, inc=1,
                    device_id={"cell": near(k), "gene": lax.rem(gene + g, genes)},
                    device_id_type=MESH,
                )
                greeted += 1
    for k in range(1, outer):
        pl.semaphore_signal(barrier, inc=1, device_id={"cell": far(k)}, device_id_type=MESH)
        greeted += 1

    held[slots] = jnp.zeros((side, side), held.dtype)
    for copy in slot_copies:
        copy.wait()
    places = (cell_dev // side) * gene_blocks
    lane = lax.broadcasted_iota(jnp.int32, (1, slots), 1)
    spots = jnp.where(
        lane < slot_count[0, 0], slots_in[0] * gene_blocks + slots_in[1], places
    )
    square = (slots, slots)
    turned = jnp.where(diagonal(slots), jnp.broadcast_to(spots, square), 0)
    turned = jnp.sum(turned, axis=1, keepdims=True)
    flat = (slots, places)
    found = jnp.broadcast_to(turned, flat) == lax.broadcasted_iota(jnp.int32, flat, 1)
    found = jnp.where(found, lax.broadcasted_iota(jnp.int32, flat, 0), slots)
    places_out[...] = jnp.min(found, axis=0, keepdims=True)
    listing = pltpu.make_async_copy(places_out, table, table_sem)
    listing.start()
    listing.wait()
    fetch.wait()
    first_basis.wait()

    def remote(source, target, send_sem, recv_sem, **device):
        return pltpu.make_async_remote_copy(
            src_ref=source, dst_ref=target, send_sem=send_sem, recv_sem=recv_sem,
            device_id=device, device_id_type=MESH,
        )

    def pair_copy(it, r):
        return remote(
            mine.at[it, r], theirs.at[it, r], pair_send.at[0], pair_recv.at[it, r], gene=other
        )

    def gram_copy(it, k):
        return remote(
            grams.at[it, spot], grams.at[it, spot], gram_send.at[0], gram_recv.at[it],
            cell=near(k), gene=head,
        )

    def plane_copy(it, k):
        return remote(
            planes.at[it, here], planes.at[it, here], plane_send.at[0], plane_recv.at[it],
            cell=far(k),
        )

    def near_copy(it, group, k):
        return remote(
            codes_out.at[it, group, k], codes_in.at[it, gene, group, k],
            near_send.at[0], near_recv.at[gene, group], cell=near(k), gene=head,
        )

    def step_copy(it, group, k):
        return remote(
            steps_out.at[it, group, k], steps_in.at[it, gene, group, k],
            step_send.at[0], step_recv.at[gene, group], cell=near(k), gene=head,
        )

    def line_copy(it, k):
        return remote(
            lines_out.at[it], lines_in.at[it, gene, k],
            line_send.at[0], line_recv.at[it, gene], cell=near(k), gene=head,
        )

    def far_copy(it, group):
        return remote(
            far_out.at[it, group], far_in.at[it, here],
            far_send.at[0], far_recv.at[it], cell=group * inner + spot,
        )

    def fars_copy(it, group):
        return remote(
            fars_out.at[it, group], fars_in.at[it, here],
            fars_send.at[0], fars_recv.at[it], cell=group * inner + spot,
        )

    def tail_copy(it, k):
        return remote(
            tails_out.at[it], tails_in.at[it, here],
            tail_send.at[0], tail_recv.at[it], cell=far(k),
        )

    def column_copy(target):
        return remote(
            columns.at[here], columns.at[here], column_send.at[0], column_recv.at[here],
            cell=target * inner + spot,
        )

    def mid_copy(group, g, k):
        return remote(
            columns.at[group, g], middle.at[group * inner + spot],
            mid_send.at[group], mid_recv.at[group], cell=near(k), gene=g,
        )

    def awaited(refs, sem):
        remote(refs, refs, pair_send.at[0], sem, gene=other).wait_recv()

    def drained(refs, sem):
        remote(refs, refs, sem, pair_recv.at[0, 0], gene=other).wait_send()

    def added(ref, count):
        total = ref[0]
        for c in range(1, count):
            total = total + ref[c]
        return total

    def loop(first, last, act):
        if last - first <= 4:
            for k in range(first, last):
                act(k)
        else:
            def body(k, _):
                act(k)
                return 0

            lax.fori_loop(first, last, body, 0)

    def part(r):
        return pl.ds(r * piece, piece)

    def along(m):
        return lax.rem(here + jnp.where(2 * here < outer, m, outer - m), outer)

    def place(low, high):
        for row in range(cell_dev // side):
            for col in range(low, high):
                dense[row * side : (row + 1) * side, col * side : (col + 1) * side] = held[
                    table[0, row * gene_blocks + col]
                ]

    def score(left, r, lanes):
        return lax.dot_general(
            left, dense[part(r), lanes], (((1,), (1,)), ((), ())),
            preferred_element_type=jnp.float32,
        )

    def first_scores():
        stages = 8
        share_cols = gene_blocks // stages
        with scope("place"):
            place(0, share_cols)
        for q in range(stages):
            lanes = slice(q * share_cols * side, (q + 1) * share_cols * side)
            with scope("score"):
                if q + 1 < stages:
                    place((q + 1) * share_cols, (q + 2) * share_cols)
                for r in range(parts):
                    fresh = score(first[:, lanes], r, lanes)
                    mine[0, r] = fresh if q == 0 else mine[0, r] + fresh
                    if q == stages - 1:
                        if r == 0:
                            pl.semaphore_wait(barrier, greeted)
                        pair_copy(0, r).start()

    def second_scores():
        def step(m):
            group = along(m)
            with scope("midwait"):
                @pl.when(lead)
                def _():
                    awaited(middle.at[pl.ds(0, inner - 1)], mid_recv.at[group])
                    middle[group * inner + spot] = columns[group, head]

                @pl.when(follow)
                def _():
                    awaited(middle.at[pl.ds(0, inner)], mid_recv.at[group])

            left = jnp.concatenate([middle[group * inner + c] for c in range(inner)], axis=1)
            lanes = pl.ds(pl.multiple_of(group * span, 128), span)
            with scope("score"):
                for r in range(parts):
                    fresh = score(left, r, lanes)
                    if isinstance(m, int) and m == 0:
                        mine[1, r] = fresh
                    else:
                        mine[1, r] = mine[1, r] + fresh
                    if isinstance(m, int) and m == outer - 1:
                        pair_copy(1, r).start()

        step(0)
        loop(1, outer - 1, step)
        step(outer - 1)

    def share(group):
        for k in list(range(1, inner)) + [0]:
            for g in range(genes):
                if k > 0 or g != head:
                    mid_copy(group, g, k).start()

    def iteration(it):
        if it == 0:
            first_scores()
        else:
            second_scores()

        with scope("merge"):
            peak = None
            for r in range(parts):
                pair_copy(it, r).wait_recv()
                whole = mine[it, r] + theirs[it, r]
                most = jnp.max(jnp.abs(whole), axis=1, keepdims=True)
                peak = most if peak is None else jnp.maximum(peak, most)
                pieces = split_three(whole)
                for i in range(it + 2):
                    stacked[i * width : (i + 1) * width, part(r)] = pieces[i]

            peak = jnp.maximum(peak, 1e-30)
            lines_out[it] = turn(peak)
            shrink = jnp.broadcast_to(1.0 / peak, (width, chunk))
            for k in range(1, inner):
                line_copy(it, k).start()

            @pl.when(follow)
            def _():
                line_copy(it, 0).start()

        def gram():
            whole = stacked[0 : (it + 2) * width, :]
            cross = lax.dot_general(
                whole, whole, (((1,), (1,)), ((), ())), preferred_element_type=jnp.float32
            )
            cross = sum(cross[i * width : (i + 1) * width] for i in range(it + 2))
            total = sum(cross[:, i * width : (i + 1) * width] for i in range(it + 2))
            grams[it, spot] = jnp.concatenate([total[:half], total[half:]], axis=1)
            for k in range(inner):
                gram_copy(it, k).start()

        def product(lanes):
            wide = jnp.dot(
                stacked[0 : 2 * width, :], dense[:, lanes], preferred_element_type=jnp.float32
            )
            return wide[:width] + wide[width:]

        def dispatch(group, k, value):
            coded, steps = encode(value * shrink)
            codes_out[it, group, k] = coded
            steps_out[it, group, k] = steps

        def send(group, k):
            step_copy(it, group, k).start()
            near_copy(it, group, k).start()

        def multiply(m):
            group = along(outer - m)

            def by_chunk():
                for k in list(range(1, inner)) + [0]:
                    at = (group * inner + lax.rem(spot + k, inner)) * chunk
                    value = product(pl.ds(pl.multiple_of(at, side), chunk))
                    dispatch(group, k, value)
                    send(group, k)

            def whole_group():
                wide = product(pl.ds(pl.multiple_of(group * span, 128), span))
                for c in range(inner):
                    sums_near[group, c] = wide[:, c * chunk : (c + 1) * chunk]
                for k in range(inner):
                    dispatch(group, k, sums_near[group, lax.rem(spot + k, inner)])
                for k in range(1, inner):
                    send(group, k)

            if isinstance(m, int) and m == 1 and chunk % side == 0:
                pl.when(follow)(by_chunk)

                @pl.when(lead)
                def _():
                    whole_group()

                return
            whole_group()

            @pl.when(follow)
            def _():
                send(group, 0)

        def forward(m):
            group = along(outer - m)
            own = isinstance(m, int) and m == outer
            for g in range(genes):
                low = 1 if g == head else 0
                awaited(steps_in.at[it, g, group, pl.ds(low, inner - low)], step_recv.at[g, group])
                awaited(codes_in.at[it, g, group, pl.ds(low, inner - low)], near_recv.at[g, group])
                total = sums_near[group, spot] if g == head else None
                for k in range(low, inner):
                    value = decode(codes_in[it, g, group, k], steps_in[it, g, group, k]) * factors[g, k]
                    total = value if total is None else total + value
                if own:
                    sums_own[g] = total
                else:
                    coded, steps = encode(total * gains[g])
                    far_out[it, group, g] = coded
                    fars_out[it, group, g] = steps
            if not own:
                fars_copy(it, group).start()
                far_copy(it, group).start()

        def reduce():
            with scope("lines"):
                for g in range(genes):
                    low = 1 if g == head else 0
                    awaited(lines_in.at[it, g, pl.ds(low, inner - low)], line_recv.at[it, g])
                    tail = lines_out[it] if g == head else None
                    for k in range(low, inner):
                        line = lines_in[it, g, k]
                        tail = line if tail is None else tail + line
                        factors[g, k] = turn_back(line, chunk)
                    tails_out[it, g] = tail
                    gains[g] = turn_back(1.0 / tail, chunk)
                for k in range(1, outer):
                    tail_copy(it, k).start()
            with scope("gramwait"):
                awaited(grams.at[it], gram_recv.at[it])
            planes[it, here] = added(grams.at[it], inner)
            for k in range(1, outer):
                plane_copy(it, k).start()
            with scope("forward"):
                loop(1, outer, forward)
                forward(outer)
            awaited(tails_in.at[it, pl.ds(0, outer - 1)], tail_recv.at[it])
            for g in range(genes):
                for k in range(1, outer):
                    stretch[g, k] = turn_back(tails_in[it, lax.rem(here + k, outer), g], chunk)
            with scope("planewait"):
                awaited(planes.at[it, pl.ds(0, outer - 1)], plane_recv.at[it])
            total = added(planes.at[it], outer)
            total = jnp.concatenate([total[:, :width], total[:, width:]], axis=0)
            with scope("inverse"):
                inverse = inverse_factor(total)
            if it == 1:
                factor[...] = inverse
                remote(factor, factor, factor_send.at[0], factor_recv.at[0], gene=other).start()
            with scope("farwait"):
                awaited(fars_in.at[it, pl.ds(0, outer - 1)], fars_recv.at[it])
                awaited(far_in.at[it, pl.ds(0, outer - 1)], far_recv.at[it])
            with scope("result"):
                summed = []
                for g in range(genes):
                    part_sum = sums_own[g]
                    for k in range(1, outer):
                        source = lax.rem(here + k, outer)
                        value = decode(far_in[it, source, g], fars_in[it, source, g])
                        part_sum = part_sum + value * stretch[g, k]
                    summed.append(part_sum)
                summed = jnp.concatenate(summed, axis=1)
                result = jnp.dot(
                    inverse, summed, precision=HIGH, preferred_element_type=jnp.float32
                )
                result = [result[:, g * chunk : (g + 1) * chunk] for g in range(genes)]
                if it == 0:
                    for g in range(genes):
                        columns[here, g] = result[g].astype(columns.dtype)
                    for m in range(outer - 1, 0, -1):
                        column_copy(along(m)).start()
                    share(here)
                else:
                    load_res[...] = result[0]
                    remote(load_res, load_in, load_send.at[0], load_recv.at[0], gene=other).start()
                    load_out[...] = result[head]
            if it == 0:
                def relay(m):
                    group = along(m)
                    with scope("columnwait"):
                        awaited(columns.at[group], column_recv.at[group])
                    share(group)

                loop(1, outer, relay)

        with scope("gram"):
            pl.when(follow)(gram)
        with scope("multiply"):
            loop(1, outer + 1, multiply)
        pl.when(lead)(reduce)

    iteration(0)
    iteration(1)

    @pl.when(follow)
    def _():
        with scope("factorwait"):
            awaited(factor, factor_recv.at[0])

    with scope("finish"):
        scale = jnp.sqrt(jnp.float32(cells * cell_dev))
        left = jnp.concatenate(
            [jnp.concatenate([p] * 3, axis=1) for p in split_three(factor[...])], axis=0
        )
        for r in range(parts):
            final = jnp.dot(left, stacked[:, part(r)], preferred_element_type=jnp.float32)
            final = final[:width] + final[width : 2 * width] + final[2 * width :]
            basis_out[:, part(r)] = (final * scale).astype(basis_out.dtype)

    @pl.when(follow)
    def _():
        with scope("loadwait"):
            awaited(load_in, load_recv.at[0])
        load_out[...] = load_in[...]
        drained(codes_out, near_send.at[0])
        drained(steps_out, step_send.at[0])
        drained(grams, gram_send.at[0])
        drained(lines_in.at[:, 0], line_send.at[0])

    @pl.when(lead)
    def _():
        drained(codes_out.at[:, :, pl.ds(1, inner - 1)], near_send.at[0])
        drained(steps_out.at[:, :, pl.ds(1, inner - 1)], step_send.at[0])
        drained(lines_in.at[:, 0, pl.ds(1, inner - 1)], line_send.at[0])
        drained(planes.at[:, pl.ds(0, outer - 1)], plane_send.at[0])
        drained(far_in.at[:, pl.ds(0, outer - 1)], far_send.at[0])
        drained(fars_in.at[:, pl.ds(0, outer - 1)], fars_send.at[0])
        drained(tails_in.at[:, pl.ds(0, outer - 1)], tail_send.at[0])
        drained(columns.at[pl.ds(0, outer - 1)], column_send.at[0])
        loop(0, outer, lambda group: drained(
            middle.at[pl.ds(0, inner * genes - 1)], mid_send.at[group]
        ))
        drained(factor, factor_send.at[0])
        drained(load_res, load_send.at[0])

    drained(mine, pair_send.at[0])


def local(cells, genes, tiles, tile_row, tile_col, tile_count, start_basis):
    slots, side = tiles.shape[1], tiles.shape[-1]
    width, gene_dev = start_basis.shape
    gene_blocks = gene_dev // side
    cell_dev = ROW_BLOCKS * side
    chunk = gene_dev // cells
    parts = 2
    inner = 1
    while inner * inner * 4 <= cells and cells % (inner * 2) == 0:
        inner = inner * 2
    outer = cells // inner
    places = ROW_BLOCKS * gene_blocks
    dma = pltpu.SemaphoreType.DMA
    shapes = (
        jax.ShapeDtypeStruct((width, cell_dev), jnp.bfloat16),
        jax.ShapeDtypeStruct((width, chunk), jnp.float32),
    )
    results = pl.pallas_call(
        functools.partial(kernel, cells, inner, genes, parts),
        out_shape=shapes,
        in_specs=[
            pl.BlockSpec(memory_space=pltpu.SMEM),
            pl.BlockSpec(memory_space=pltpu.HBM),
            pl.BlockSpec(memory_space=pltpu.HBM),
            pl.BlockSpec(memory_space=pltpu.HBM),
            pl.BlockSpec(memory_space=pltpu.HBM),
        ],
        out_specs=(
            pl.BlockSpec(memory_space=pltpu.VMEM),
            pl.BlockSpec(memory_space=pltpu.VMEM),
        ),
        scratch_shapes=[
            pltpu.VMEM((2, 1, slots), jnp.int32),
            pltpu.VMEM((1, places), jnp.int32),
            pltpu.SMEM((1, places), jnp.int32),
            pltpu.VMEM((slots + 1, side, side), jnp.bfloat16),
            pltpu.VMEM((cell_dev, gene_dev), jnp.bfloat16),
            pltpu.VMEM((width, gene_dev), jnp.bfloat16),
            pltpu.VMEM((2, parts, width, cell_dev // parts), jnp.float32),
            pltpu.VMEM((2, parts, width, cell_dev // parts), jnp.float32),
            pltpu.VMEM((3 * width, cell_dev), jnp.bfloat16),
            pltpu.VMEM((2, inner, width // 2, 2 * width), jnp.float32),
            pltpu.VMEM((2, outer, width // 2, 2 * width), jnp.float32),
            pltpu.VMEM((width, width), jnp.float32),
            pltpu.VMEM((outer, inner, width, chunk), jnp.float32),
            pltpu.VMEM((2, outer, inner, width, chunk), jnp.int16),
            pltpu.VMEM((2, genes, outer, inner, width, chunk), jnp.int16),
            pltpu.VMEM((2, outer, inner, 1, chunk), jnp.float32),
            pltpu.VMEM((2, genes, outer, inner, 1, chunk), jnp.float32),
            pltpu.VMEM((2, 1, width), jnp.float32),
            pltpu.VMEM((2, genes, inner, 1, width), jnp.float32),
            pltpu.VMEM((genes, inner, width, chunk), jnp.float32),
            pltpu.VMEM((genes, width, chunk), jnp.float32),
            pltpu.VMEM((2, outer, genes, width, chunk), jnp.int16),
            pltpu.VMEM((2, outer, genes, width, chunk), jnp.int16),
            pltpu.VMEM((2, outer, genes, 1, chunk), jnp.float32),
            pltpu.VMEM((2, outer, genes, 1, chunk), jnp.float32),
            pltpu.VMEM((2, genes, 1, width), jnp.float32),
            pltpu.VMEM((2, outer, genes, 1, width), jnp.float32),
            pltpu.VMEM((genes, width, chunk), jnp.float32),
            pltpu.VMEM((genes, outer, width, chunk), jnp.float32),
            pltpu.VMEM((outer, genes, width, chunk), jnp.bfloat16),
            pltpu.VMEM((cells, width, chunk), jnp.bfloat16),
            pltpu.VMEM((width, chunk), jnp.float32),
            pltpu.VMEM((width, chunk), jnp.float32),
            dma, dma((2,)), dma, dma,
            dma((1,)), dma((2, parts)),
            dma((1,)), dma((2,)), dma((1,)), dma((2,)), dma((1,)), dma((1,)),
            dma((1,)), dma((genes, outer)), dma((1,)), dma((genes, outer)),
            dma((1,)), dma((2, genes)),
            dma((1,)), dma((2,)), dma((1,)), dma((2,)), dma((1,)), dma((2,)),
            dma((1,)), dma((outer,)), dma((outer,)), dma((outer,)), dma((1,)), dma((1,)),
        ],
        compiler_params=pltpu.CompilerParams(
            collective_id=0, has_side_effects=True, vmem_limit_bytes=44 * 1024 * 1024
        ),
    )(tile_count, *(
        pltpu.with_memory_space_constraint(array, pltpu.HBM)
        for array in (tile_row, tile_col, tiles[0], start_basis)
    ))
    return pl.pallas_call(
        deliver,
        out_shape=shapes,
        in_specs=[pl.BlockSpec(memory_space=pltpu.VMEM)] * 2,
        out_specs=(pl.BlockSpec(memory_space=pl.ANY),) * 2,
        scratch_shapes=[dma((2,))],
        compiler_params=pltpu.CompilerParams(vmem_limit_bytes=1024 * 1024),
    )(*results)


def deliver(basis, load, basis_out, load_out, sems):
    copies = [
        pltpu.make_async_copy(basis, basis_out, sems.at[0]),
        pltpu.make_async_copy(load, load_out, sems.at[1]),
    ]
    for copy in copies:
        copy.start()
    for copy in copies:
        copy.wait()


def solution(mesh):
    return jax.shard_map(
        functools.partial(local, mesh.shape["cell"], mesh.shape["gene"]),
        mesh=mesh,
        in_specs=(
            P("gene", "cell", None, None),
            P("gene", "cell"),
            P("gene", "cell"),
            P("gene", "cell"),
            P(None, "gene"),
        ),
        out_specs=(P(None, "cell"), P(None, ("gene", "cell"))),
        check_vma=False,
    )
```
